32 devices in a mesh: dp: 1 (over z), tp: 32 (over x, y, core).
Axes of the slice: x: 4, y: 4, z: 1, core: 2. Of those that a mesh axis runs over, the one named last changes fastest.
The devices are a block of a 4x4x8 slice.
Arguments:
- x: bfloat16 [4096, 8192], P(('dp', 'tp'))
- w_gate: bfloat16 [8192, 49152], P(None, 'tp')
- w_up: bfloat16 [8192, 49152], P(None, 'tp')
- w_down: bfloat16 [49152, 8192], P('tp')
Outputs:
- output: bfloat16 [4096, 8192], P(('dp', 'tp'))
All inputs are finite; a program needn't handle non-finite values.
Results may differ from the reference program's by a relative error of at most 0.016.
Values are sent between devices in bfloat16 or wider.
A program may use at most 768 MiB of HBM per device.

```python
import jax
import jax.numpy as jnp

ROWS = 4096
D = 8192
FF = 49152


def setup_inputs(seed: int = 0, part: int = 0) -> dict:
    kx, kg, ku, kd = jax.random.split(jax.random.key(seed), 4)
    drawn = {
        "x": jax.random.normal(jax.random.fold_in(kx, part), (ROWS, D), jnp.float32),
        "w_gate": jax.random.normal(kg, (D, FF), jnp.float32) * D**-0.5,
        "w_up": jax.random.normal(ku, (D, FF), jnp.float32) * D**-0.5,
        "w_down": jax.random.normal(kd, (FF, D), jnp.float32) * FF**-0.5,
    }
    return {k: v.astype(jnp.bfloat16) for k, v in drawn.items()}


def reference(x, w_gate, w_up, w_down):
    gate = jnp.dot(x, w_gate, preferred_element_type=jnp.float32)
    up = jnp.dot(x, w_up, preferred_element_type=jnp.float32)
    hidden = (jax.nn.silu(gate) * up).astype(jnp.bfloat16)
    return jnp.dot(hidden, w_down, preferred_element_type=jnp.float32).astype(jnp.bfloat16)
```

```python
import functools
import math

import jax
import jax.numpy as jnp
from jax import lax
from jax.experimental import pallas as pl
from jax.experimental.pallas import tpu as pltpu
from jax.sharding import PartitionSpec as P

F32, BF16 = jnp.float32, jnp.bfloat16


def kernel(side, tn, dt, x, wg, wu, wd, y, xs, wp, rs, wbuf, h0, hk, hs, out, inb, ab, bb, wsem, xsem, isem, ysem,
           ag_s, ag_r, pu_s, pu_r, wp_s, wp_r, hx_s, hx_r, rs_s, rs_r, a_s, a_r, b_s, b_r, hfree):
    rows, d = x.shape
    hid = wg.shape[1]
    hr = rows // 2
    half_rows = side * hr
    nt, nd = hid // tn, d // dt
    sub = dt // tn
    part_cols = hid // 2
    wp_rows = hid // nt

    t = lax.axis_index("tp")
    c = lax.rem(t, 2)
    cx, cy = t // (2 * side), lax.rem(t // 2, side)
    f, s = cx * (1 - c) + cy * c, cy * (1 - c) + cx * c

    def at(df, ds):
        ff, ss = lax.rem(f + df + side, side), lax.rem(s + ds + side, side)
        return ((ff * (1 - c) + ss * c) * side + ss * (1 - c) + ff * c) * 2 + c

    fp, fm, sp, sm, sib = at(1, 0), at(-1, 0), at(0, 1), at(0, -1), t + 1 - 2 * c

    def remote(src, dst, send, recv, dev):
        return pltpu.make_async_remote_copy(src_ref=src, dst_ref=dst, send_sem=send, recv_sem=recv, device_id={"tp": dev})

    def when(cond):
        return pl.when(cond)

    def row0(j, hf):
        return hf * half_rows + j * hr

    def piece(k, j, hf, other=0):
        return xs.at[other, k, pl.ds(row0(j, hf), hr)]

    def source(k, j, hf):
        if isinstance(k, int) and isinstance(j, int) and k == 0 and j == 0:
            return x.at[pl.ds(hf * hr, hr)]
        return piece(k, j, hf)

    def move(src, k, j, hf, dev):
        i = j * 2 + hf
        return remote(src, piece(k, j, hf), ag_s.at[k, i], ag_r.at[k, i], dev)

    def hand(k, j, hf):
        i = j * 2 + hf
        return remote(source(k, j, hf), piece(k, j, hf, 1), pu_s.at[k, i], pu_r.at[k, i], sib)

    def arrive(k, j, hf):
        move(piece(k, j, hf), k, j, hf, sib).wait_recv()
        hand(k, j, hf).start()

    def push(k, j):
        for hf in range(2):
            arrive(k, j, hf)

    def forward(k, j):
        for hf, dev in ((0, sp), (1, sm)):
            move(source(k, j, hf), k + 1, j, hf, dev).start()

    def far():
        move(piece(0, 1, 0), 0, 3, 0, fp).start()
        move(piece(0, 2, 1), 0, 3, 1, fm).start()

    def load(xb, slot, i, k, j, n):
        hf = i % 2
        seg = n * hr
        if i < 2:
            src = x.at[pl.ds(hf * hr, hr)] if n == 1 and isinstance(j, int) and j == 0 else xs.at[0, k, pl.ds(row0(j, hf), seg)]
        else:
            src = xs.at[1, k, pl.ds(row0(j, hf), seg)]
        return pltpu.make_async_copy(src, xb.at[slot, pl.ds(i * seg, seg)], xsem.at[slot, i])

    def load_start(xb, slot, i, k, j, n):
        if i >= 2:
            for q in range(n):
                hand(k, j + q, i % 2).wait_recv()
        load(xb, slot, i, k, j, n).start()

    def u_copies(n, slot):
        cols = pl.ds(pl.multiple_of(n * tn, tn), tn)
        return [pltpu.make_async_copy(w.at[:, cols], wbuf.at[slot, i], wsem.at[slot, i]) for i, w in enumerate((wg, wu))]

    def d_rows(q):
        return q // 2, (q % 2) * 2 * hid

    def d_copies(n, slot):
        r = []
        for q in range(sub):
            p, o = d_rows(q)
            cols = pl.ds(pl.multiple_of(n * dt + q * tn, tn), tn)
            for i, w in enumerate((wd, wp)):
                r.append(pltpu.make_async_copy(w.at[:, cols], wbuf.at[slot, p, pl.ds(o + i * hid, hid)], wsem.at[slot, 2 * q + i]))
        return r

    def start(copies):
        for cp in copies:
            cp.start()

    def wait(copies):
        for cp in copies:
            cp.wait()

    def h_copy(hdst, slot, j, n, part, hf, idx):
        seg, i = n * hr, part * 2 + hf
        cols = part * part_cols
        return remote(hs.at[slot, pl.ds(hf * seg, seg), pl.ds(cols, part_cols)],
                      hdst.at[pl.ds(row0(j, hf), seg), pl.ds(hid + cols, part_cols)],
                      hx_s.at[slot, i], hx_r.at[idx, i], sib)

    def h_push(hdst, slot, j, n, part, idx):
        for hf in range(2):
            h_copy(hdst, slot, j, n, part, hf, idx).start()

    def h_sent(slot, n):
        for part in range(2):
            for hf in range(2):
                h_copy(h0, slot, 0, n, part, hf, 0).wait_send()

    def h_here(idx, n):
        for part in range(2):
            for hf in range(2):
                h_copy(h0, 0, 0, n, part, hf, idx).wait_recv()

    def u_phase(xb, slot, hdst, j, n, idx, hook, nxt):
        seg = n * hr
        m = 4 * seg

        def body(i, carry):
            ws = lax.rem(i, 2)
            hook(i)

            @when(i == nt // 2)
            def _():
                h_push(hdst, slot, j, n, 0, idx)

            @when(i < nt - 1)
            def _():
                start(u_copies(i + 1, 1 - ws))

            @when(i == nt - 1)
            def _():
                nxt()

            @when(i == 0)
            def _():
                for q in range(4):
                    load(xb, slot, q, 0, 1, n).wait()

            wait(u_copies(i, ws))
            lhs = xb.at[slot, pl.ds(0, m)]
            gate = jnp.dot(lhs[...], wbuf[ws, 0], preferred_element_type=F32)
            up = jnp.dot(lhs[...], wbuf[ws, 1], preferred_element_type=F32)
            hidden = (jax.nn.silu(gate) * up).astype(BF16)
            cols = pl.ds(pl.multiple_of(i * tn, tn), tn)
            for hf in range(2):
                hdst[pl.ds(row0(j, hf), seg), cols] = hidden[hf * seg : (hf + 1) * seg]
            hs[slot, pl.ds(0, 2 * seg), cols] = hidden[2 * seg :]
            return carry

        lax.fori_loop(0, nt, body, 0)
        h_push(hdst, slot, j, n, 1, idx)

    def sum_copy(hop, n, hf):
        part = pl.ds(hf * half_rows, half_rows)
        return remote(out.at[n, part], rs.at[hop, n, part], rs_s.at[n, hf], rs_r.at[hop, 2 * n + hf], (sp, sm)[hf])

    def in_copy(hop, n):
        b = lax.rem(n, 2)
        return pltpu.make_async_copy(rs.at[hop, n], inb.at[b], isem.at[b])

    def in_start(hop, n):
        for hf in range(2):
            sum_copy(hop, n, hf).wait_recv()
        in_copy(hop, n).start()

    def products(h, n, q):
        p, o = d_rows(q)
        ws = lax.rem(n, 2)
        cols = slice(q * tn, (q + 1) * tn)
        term = jnp.dot(h[...], wbuf[ws, p, pl.ds(o, 2 * hid)], preferred_element_type=F32)
        return term + inb[lax.rem(n, 2), :, cols].astype(F32), cols

    def a_copy(n, hf):
        return remote(out.at[n, pl.ds(hf * hr, hr)], ab.at[n, hf], a_s.at[n, hf], a_r.at[n, hf], (fp, fm)[hf])

    def b_copy(n, i):
        return remote(out.at[n, pl.ds((1 + i) * rows, rows)], bb.at[n, i], b_s.at[n, i], b_r.at[n, i], (fp, fm)[i])

    def y_copy(n):
        cols = pl.ds(pl.multiple_of(n * dt, dt), dt)
        return pltpu.make_async_copy(out.at[n, pl.ds(3 * rows, rows)], y.at[:, cols], ysem.at[n])

    start(u_copies(0, 0))
    barrier = pltpu.get_barrier_semaphore()
    for dev in (fp, fm, sp, sm, sib):
        pl.semaphore_signal(barrier, 1, device_id={"tp": dev})
    pl.semaphore_wait(barrier, 5)

    for hf in range(2):
        hand(0, 0, hf).start()
    for hf in range(2):
        move(source(0, 0, hf), 0, 1, hf, fp).start()
        move(source(0, 0, hf), 0, 2, hf, fm).start()
    inb[...] = jnp.zeros_like(inb)

    def rounds(xb):
        for i in range(4):
            load_start(xb, 0, i, 0, 0, 1)

        def hook(i):
            @when(i == nt - 2)
            def _():
                arrive(0, 1, 0)
                arrive(0, 2, 0)

        u_phase(xb, 0, h0, 0, 1, 0, hook, lambda: start(u_copies(0, 0)))

        arrive(0, 1, 1)
        arrive(0, 2, 1)
        for j in range(3):
            forward(0, j)
        for i in range(4):
            load_start(xb, 1, i, 0, 1, 2)

        def hook(i):
            @when(i == 3)
            def _():
                push(1, 0)

            @when(i == 4)
            def _():
                far()

            @when(i == 5)
            def _():
                push(1, 1)

        u_phase(xb, 1, h0, 1, 2, 1, hook, lambda: start(u_copies(0, 0)))
        for i in range(4):
            load_start(xb, 0, i, 1, 0, 2)

        def one_round(k, carry):
            def chunk(b, carry):
                @when((k == 1) & (b == 0))
                def _():
                    h_sent(0, 1)

                @when((k > 1) | (b == 1))
                def _():
                    h_sent(b, 2)

                @when((k == 1) & (b == 1))
                def _():
                    push(1, 3)
                    for i in range(4):
                        load_start(xb, 1, i, 1, 2, 2)

                def hook(i):
                    @when((k == 1) & (b == 0))
                    def _():
                        piece_rows = pl.ds(i * wp_rows, wp_rows)
                        remote(wd.at[piece_rows], wp.at[piece_rows], wp_s.at[i], wp_r.at[i], sib).start()

                        @when(i == 3)
                        def _():
                            push(0, 3)
                            forward(0, 3)

                        @when(i == 4)
                        def _():
                            push(1, 2)
                            forward(1, 0)

                        @when(i == 5)
                        def _():
                            forward(1, 1)

                    @when((k == 1) & (b == 1))
                    def _():
                        @when(i == 0)
                        def _():
                            forward(1, 2)

                        @when(i == 1)
                        def _():
                            forward(1, 3)

                        @when(i == 3)
                        def _():
                            push(2, 0)

                        @when(i == 5)
                        def _():
                            push(2, 1)
                            forward(2, 0)

                    @when((k == 2) & (b == 1))
                    def _():
                        @when(i == 1)
                        def _():
                            push(3, 0)

                        @when(i == 3)
                        def _():
                            push(3, 1)

                        @when(i == 5)
                        def _():
                            push(3, 2)

                    @when((k > 1) & (b == 0))
                    def _():
                        @when(i == nt // 2)
                        def _():
                            pl.semaphore_wait(hfree, 1)

                        for q in range(4):
                            @when(i == 2 + q)
                            def _():
                                load_start(xb, 1, q, k, 2, 2)

                    @when((k > 1) & (b == 1) & (i == nt - 2))
                    def _():
                        in_start(k - 2, 0)

                def nxt():
                    @when(b == 0)
                    def _():
                        start(u_copies(0, 0))

                    @when(b == 1)
                    def _():
                        @when(k == 1)
                        def _():
                            for i in range(nt):
                                piece_rows = pl.ds(i * wp_rows, wp_rows)
                                remote(wd.at[piece_rows], wp.at[piece_rows], wp_s.at[i], wp_r.at[i], sib).wait_recv()

                        start(d_copies(0, 0))

                u_phase(xb, b, hk, 2 * b, 2, 2 + b, hook, nxt)
                return carry

            lax.fori_loop(0, 2, chunk, 0)
            h_here(2, 2)
            h_here(3, 2)

            def down(n, carry):
                ws = lax.rem(n, 2)

                @when(n < nd - 1)
                def _():
                    start(d_copies(n + 1, 1 - ws))

                @when(n == nd - 1)
                def _():
                    start(u_copies(0, 0))

                @when(k > 1)
                def _():
                    in_copy(k - 2, n).wait()

                    @when(n < nd - 1)
                    def _():
                        in_start(k - 2, n + 1)

                    for hf in range(2):
                        sum_copy(0, n, hf).wait_send()

                @when(k == 1)
                def _():
                    @when(n == 1)
                    def _():
                        push(2, 2)
                        forward(2, 1)

                    @when(n == 3)
                    def _():
                        forward(2, 2)

                    @when(n == 5)
                    def _():
                        push(2, 3)
                        forward(2, 3)

                @when((k == 2) & (n == 1))
                def _():
                    push(3, 3)

                @when(k < 3)
                def _():
                    for q in range(4):
                        @when(n == 2 + q)
                        def _():
                            load_start(xb, 0, q, k + 1, 0, 2)

                @when(k == 3)
                def _():
                    for q in range(4):
                        @when(n == 2 + q)
                        def _():
                            load_start(xb, 0, q, 0, 3, 1)

                wait(d_copies(n, ws))
                for q in range(sub):
                    total, cols = products(hk, n, q)
                    out[n, :, cols] = total.astype(BF16)
                for hf in range(2):
                    sum_copy(k - 1, n, hf).start()
                return carry

            lax.fori_loop(0, nd, down, 0)

            @when(k < 3)
            def _():
                pl.semaphore_signal(hfree, 1, device_id={"tp": sib})

            return carry

        lax.fori_loop(1, side, one_round, 0)

        def hook(i):
            @when(i == nt - 2)
            def _():
                in_start(2, 0)

        h_sent(0, 2)
        u_phase(xb, 0, h0, 3, 1, 4, hook, lambda: start(d_copies(0, 0)))

    pl.run_scoped(rounds, pltpu.VMEM((2, 8 * hr, d), BF16))

    def last(t0, t1, t2):
        h_here(0, 1)
        h_here(1, 2)
        h_here(4, 1)

        def add_far(n):
            for hf in range(2):
                a_copy(n, hf).wait_recv()
            out[n, pl.ds(rows, hr)] = (t2[n, :hr] + ab[n, 0].astype(F32)).astype(BF16)
            out[n, pl.ds(rows + hr, hr)] = t2[n, hr:].astype(BF16)
            out[n, pl.ds(2 * rows, hr)] = t1[n, :hr].astype(BF16)
            out[n, pl.ds(2 * rows + hr, hr)] = (t1[n, hr:] + ab[n, 1].astype(F32)).astype(BF16)
            for i in range(2):
                b_copy(n, i).start()

        def add_near(n):
            for i in range(2):
                b_copy(n, i).wait_recv()
            out[n, pl.ds(3 * rows, rows)] = (t0[n] + bb[n, 0].astype(F32) + bb[n, 1].astype(F32)).astype(BF16)
            y_copy(n).start()

        def down(n, carry):
            ws = lax.rem(n, 2)

            @when(n < nd - 1)
            def _():
                start(d_copies(n + 1, 1 - ws))

            in_copy(2, n).wait()

            @when(n < nd - 1)
            def _():
                in_start(2, n + 1)

            for hf in range(2):
                sum_copy(0, n, hf).wait_send()

            @when(n >= 2)
            def _():
                add_far(n - 2)

            @when(n >= 5)
            def _():
                add_near(n - 5)

            wait(d_copies(n, ws))
            for q in range(sub):
                total, cols = products(h0, n, q)
                for hf in range(2):
                    o = hf * half_rows
                    dst = pl.ds(hf * hr, hr)
                    t0[n, dst, cols] = total[o : o + hr]
                    t1[n, dst, cols] = total[o + hr : o + 2 * hr]
                    t2[n, dst, cols] = total[o + 2 * hr : o + 3 * hr]
                    out[n, dst, cols] = total[o + 3 * hr : o + 4 * hr].astype(BF16)
            for hf in range(2):
                a_copy(n, hf).start()
            return carry

        lax.fori_loop(0, nd, down, 0)

        def drain(n, carry):
            @when(n < nd)
            def _():
                add_far(n)

            add_near(n - 3)
            return carry

        lax.fori_loop(nd - 2, nd + 3, drain, 0)

    shape = pltpu.VMEM((nd, rows, dt), F32)
    pl.run_scoped(last, shape, shape, shape)

    for n in range(nd):
        y_copy(n).wait()
        for i in range(2):
            a_copy(n, i).wait_send()
            b_copy(n, i).wait_send()
    h_sent(0, 1)
    h_sent(1, 2)
    for i in range(nt):
        piece_rows = pl.ds(i * wp_rows, wp_rows)
        remote(wd.at[piece_rows], wp.at[piece_rows], wp_s.at[i], wp_r.at[i], sib).wait_send()
    for k in range(side):
        for j in range(side):
            for hf in range(2):
                hand(k, j, hf).wait_send()
                if k or j:
                    move(piece(k, j, hf), k, j, hf, sib).wait_send()


def build(mesh, tn, dt):
    side = math.isqrt(mesh.shape["tp"] // 2)

    def step(x, w_gate, w_up, w_down):
        rows, d = x.shape
        hid = w_gate.shape[1]
        hr = rows // 2
        nt, nd = hid // tn, d // dt
        dma = pltpu.SemaphoreType.DMA
        hbm = pl.BlockSpec(memory_space=pltpu.HBM)
        m = side * rows
        result = pl.pallas_call(
            functools.partial(kernel, side, tn, dt),
            out_shape=(
                jax.ShapeDtypeStruct((rows, d), BF16),
                jax.ShapeDtypeStruct((2, side, m, d), BF16),
                jax.ShapeDtypeStruct((hid, d), BF16),
                jax.ShapeDtypeStruct((side - 1, nd, m, dt), BF16),
            ),
            in_specs=[hbm] * 4,
            out_specs=[hbm] * 4,
            scratch_shapes=[
                pltpu.VMEM((2, 2, d, tn), BF16),
                pltpu.VMEM((m, 2 * hid), BF16),
                pltpu.VMEM((m, 2 * hid), BF16),
                pltpu.VMEM((2, 4 * hr, hid), BF16),
                pltpu.VMEM((nd, m, dt), BF16),
                pltpu.VMEM((2, m, dt), BF16),
                pltpu.VMEM((nd, 2, hr, dt), BF16),
                pltpu.VMEM((nd, 2, rows, dt), BF16),
                dma((2, 2 * dt // tn)),
                dma((2, 4)),
                dma((2,)),
                dma((nd,)),
                dma((side, 2 * side)),
                dma((side, 2 * side)),
                dma((side, 2 * side)),
                dma((side, 2 * side)),
                dma((nt,)),
                dma((nt,)),
                dma((2, 4)),
                dma((5, 4)),
                dma((nd, 2)),
                dma((side - 1, 2 * nd)),
                dma((nd, 2)),
                dma((nd, 2)),
                dma((nd, 2)),
                dma((nd, 2)),
                pltpu.SemaphoreType.REGULAR,
            ],
            compiler_params=pltpu.CompilerParams(collective_id=0, has_side_effects=True, vmem_limit_bytes=67043328),
            cost_estimate=pl.CostEstimate(flops=6 * side * side * 2 * rows * d * hid, bytes_accessed=9 * d * hid * 4, transcendentals=0),
            name="mlp",
        )(x, w_gate, w_up, w_down)
        return result[0]

    return jax.shard_map(
        step,
        mesh=mesh,
        in_specs=(P(("dp", "tp"), None), P(None, "tp"), P(None, "tp"), P("tp", None)),
        out_specs=P(("dp", "tp"), None),
        check_vma=False,
    )


def solution(mesh):
    return build(mesh, 256, 1024)
```

```python
import functools
import math

import jax
import jax.numpy as jnp
from jax import lax
from jax.experimental import pallas as pl
from jax.experimental.pallas import tpu as pltpu
from jax.sharding import PartitionSpec as P

F32, BF16 = jnp.float32, jnp.bfloat16


def kernel(side, tn, dt, x, wg, wu, wd, y, xs, wp, rs, wbuf, h0, hk, out, inb, wsem, xsem, isem, ysem,
           ag_s, ag_r, pu_s, pu_r, wp_s, wp_r, hx_s, hx_r, hy_s, hy_r, rs_s, rs_r, a_s, a_r, b_s, b_r, hfree, nfree):
    rows, d = x.shape
    hid = wg.shape[1]
    hr = rows // 2
    half_rows = side * hr
    m = 2 * half_rows
    seg = 2 * hr
    nt, nd = hid // tn, d // dt
    sub = dt // tn
    cuts = (0, nt // 2, nt - 1, nt)
    parts = len(cuts) - 1
    pieces = wp_s.shape[0]

    t = lax.axis_index("tp")
    c = lax.rem(t, 2)
    cx, cy = t // (2 * side), lax.rem(t // 2, side)
    f, s = cx * (1 - c) + cy * c, cy * (1 - c) + cx * c

    def at(df, ds):
        ff, ss = lax.rem(f + df + side, side), lax.rem(s + ds + side, side)
        return ((ff * (1 - c) + ss * c) * side + ss * (1 - c) + ff * c) * 2 + c

    fp, fm, sp, sm, sib = at(1, 0), at(-1, 0), at(0, 1), at(0, -1), t + 1 - 2 * c

    def remote(src, dst, send, recv, dev):
        return pltpu.make_async_remote_copy(src_ref=src, dst_ref=dst, send_sem=send, recv_sem=recv, device_id={"tp": dev})

    def when(cond):
        return pl.when(cond)

    def row0(j, hf):
        return hf * half_rows + j * hr

    def piece(k, j, hf, other=0):
        return xs.at[other, k, pl.ds(row0(j, hf), hr)]

    def source(k, j, hf):
        if isinstance(k, int) and isinstance(j, int) and k == 0 and j == 0:
            return x.at[pl.ds(hf * hr, hr)]
        return piece(k, j, hf)

    def move(src, k, j, hf, dev):
        i = j * 2 + hf
        return remote(src, piece(k, j, hf), ag_s.at[k, i], ag_r.at[k, i], dev)

    def hand(k, j, hf):
        i = j * 2 + hf
        return remote(source(k, j, hf), piece(k, j, hf, 1), pu_s.at[k, i], pu_r.at[k, i], sib)

    def arrive(k, j, hf):
        move(piece(k, j, hf), k, j, hf, sib).wait_recv()
        hand(k, j, hf).start()

    def push(k, j):
        for hf in range(2):
            arrive(k, j, hf)

    def forward(k, j):
        for hf, dev in ((0, sp), (1, sm)):
            move(source(k, j, hf), k + 1, j, hf, dev).start()

    def far(k, hf):
        move(piece(k, 1 + hf, hf), k, 3, hf, (fp, fm)[hf]).start()

    def load(xb, slot, i, src, size):
        return pltpu.make_async_copy(src, xb.at[slot, pl.ds(i * size, size)], xsem.at[slot, i])

    def load_small(xb, slot, i, k, j, hf):
        if i < 2:
            src = source(k, j, hf)
        else:
            hand(k, j, hf).wait_recv()
            src = piece(k, j, hf, 1)
        load(xb, slot, i, src, hr).start()

    def load_mid(xb, slot, i):
        other, hf = i // 2, i % 2
        if other:
            for j in (1, 2):
                hand(0, j, hf).wait_recv()
        load(xb, slot, i, xs.at[other, 0, pl.ds(row0(1, hf), seg)], seg).start()

    def load_pair(xb, slot, i, other, k, pair, hf):
        for q in range(2):
            @when(other == 1)
            def _():
                hand(k, 2 * pair + q, hf).wait_recv()
        load(xb, slot, i, xs.at[other, k, pl.ds(hf * half_rows + pair * seg, seg)], seg).start()

    def loaded(xb, slot, size):
        for i in range(4):
            load(xb, slot, i, xs.at[0, 0, pl.ds(0, size)], size).wait()

    def u_part(n, z, slot):
        cols, depth = pl.ds(pl.multiple_of(n * tn, tn), tn), pl.ds(z * (d // 2), d // 2)
        return [pltpu.make_async_copy(w.at[depth, cols], wbuf.at[slot, i, depth], wsem.at[slot, 2 * z + i])
                for i, w in enumerate((wg, wu))]

    def u_copies(n, slot):
        return u_part(n, 0, slot) + u_part(n, 1, slot)

    def d_rows(q):
        return q // 2, (q % 2) * 2 * hid

    def d_copies(n, slot):
        r = []
        for q in range(sub):
            p, o = d_rows(q)
            cols = pl.ds(pl.multiple_of(n * dt + q * tn, tn), tn)
            for i, w in enumerate((wd, wp)):
                r.append(pltpu.make_async_copy(w.at[:, cols], wbuf.at[slot, p, pl.ds(o + i * hid, hid)], wsem.at[slot, 2 * q + i]))
        return r

    def start(copies):
        for cp in copies:
            cp.start()

    def wait(copies):
        for cp in copies:
            cp.wait()

    def cut(part):
        return cuts[part] * tn, (cuts[part + 1] - cuts[part]) * tn

    def h_copy(hdst, idx, part, q, src, dst, size):
        i = part * 2 + q
        lo, width = cut(part)
        return remote(hk.at[pl.ds(m + src, size), pl.ds(lo, width)], hdst.at[pl.ds(dst, size), pl.ds(hid + lo, width)],
                      hx_s.at[idx, i], hx_r.at[idx, i], sib)

    def h_push(hdst, idx, part, src, dst, size):
        for q in range(2):
            h_copy(hdst, idx, part, q, src[q], dst[q], size).start()

    def h_sent(idx, size):
        for part in range(parts):
            for q in range(2):
                h_copy(h0, idx, part, q, 0, 0, size).wait_send()

    def h_here(idx, size):
        for part in range(parts):
            for q in range(2):
                h_copy(h0, idx, part, q, 0, 0, size).wait_recv()

    def hy_copy(part):
        lo, size = cut(part)
        return remote(hk.at[pl.ds(m, m), pl.ds(lo, size)], hk.at[pl.ds(0, m), pl.ds(hid + lo, size)],
                      hy_s.at[part], hy_r.at[part], sib)

    def w_piece(i):
        r = pl.ds(i * (hid // pieces), hid // pieces)
        return remote(wd.at[r], wp.at[r], wp_s.at[i], wp_r.at[i], sib)

    def hidden(lhs, ws):
        gate = jnp.dot(lhs[...], wbuf[ws, 0], preferred_element_type=F32)
        up = jnp.dot(lhs[...], wbuf[ws, 1], preferred_element_type=F32)
        return (jax.nn.silu(gate) * up).astype(BF16)

    def u_cols(i):
        return pl.ds(pl.multiple_of(i * tn, tn), tn)

    def u_small(xb, slot, keep, where, idx, hook, ahead, nxt):
        half = d // 2

        def body(i, carry):
            ws = lax.rem(i, 2)
            hook(i)

            for part in range(parts - 1):
                @when(i == cuts[part + 1])
                def _():
                    h_push(h0, idx, part, keep, where, hr)

            if not ahead:
                @when(i == 0)
                def _():
                    start(u_part(1, 0, 1))

            if nxt:
                start(u_part(lax.rem(i + 1, nt), 1, 1 - ws))
            else:
                @when(i < nt - 1)
                def _():
                    start(u_part(i + 1, 1, 1 - ws))

                @when(i == nt - 1)
                def _():
                    start(d_copies(0, 0))

            @when(i == 0)
            def _():
                loaded(xb, slot, hr)

            rows4 = pl.ds(0, 4 * hr)

            def products_of(z):
                wait(u_part(i, z, ws))
                lhs, depth = xb[slot, rows4, pl.ds(z * half, half)], pl.ds(z * half, half)
                return [jnp.dot(lhs, wbuf[ws, q, depth], preferred_element_type=F32) for q in range(2)]

            gate, up = products_of(0)

            if nxt == 2:
                start(u_part(lax.rem(i + 2, nt), 0, ws))
            else:
                @when(i < nt - 2 + nxt)
                def _():
                    start(u_part(lax.rem(i + 2, nt), 0, ws))

            gate2, up2 = products_of(1)
            h = (jax.nn.silu(gate + gate2) * (up + up2)).astype(BF16)
            for q in range(2):
                h0[pl.ds(where[q], hr), u_cols(i)] = h[q * hr : (q + 1) * hr]
                hk[pl.ds(m + keep[q], hr), u_cols(i)] = h[(2 + q) * hr : (3 + q) * hr]
            return carry

        lax.fori_loop(0, nt, body, 0)
        h_push(h0, idx, parts - 1, keep, where, hr)

    def u_big(xb, slot, keep, where, idx, hook):
        def body(i, carry):
            ws = lax.rem(i, 2)
            hook(i)

            for part in range(parts - 1):
                @when(i == cuts[part + 1])
                def _():
                    h_push(h0, idx, part, keep, where, seg)

            start(u_copies(lax.rem(i + 1, nt), 1 - ws))

            @when(i == 0)
            def _():
                loaded(xb, slot, seg)

            wait(u_copies(i, ws))
            h = hidden(xb.at[slot], ws)
            for q in range(2):
                h0[pl.ds(where[q], seg), u_cols(i)] = h[q * seg : (q + 1) * seg]
                hk[pl.ds(m + keep[q], seg), u_cols(i)] = h[(2 + q) * seg : (3 + q) * seg]
            return carry

        lax.fori_loop(0, nt, body, 0)
        h_push(h0, idx, parts - 1, keep, where, seg)

    def sum_copy(hop, n, hf):
        part = pl.ds(hf * half_rows, half_rows)
        return remote(out.at[n, part], rs.at[hop, n, part], rs_s.at[n, hf], rs_r.at[hop, 2 * n + hf], (sp, sm)[hf])

    def in_copy(hop, n):
        b = lax.rem(n, 2)
        return pltpu.make_async_copy(rs.at[hop, n], inb.at[b], isem.at[b])

    def in_start(hop, n):
        for hf in range(2):
            sum_copy(hop, n, hf).wait_recv()
        in_copy(hop, n).start()

    def products(h, n, q):
        p, o = d_rows(q)
        ws = lax.rem(n, 2)
        cols = slice(q * tn, (q + 1) * tn)
        term = jnp.dot(h[...], wbuf[ws, p, pl.ds(o, 2 * hid)], preferred_element_type=F32)
        return term + inb[lax.rem(n, 2), :, cols].astype(F32), cols

    def land(n, i):
        return hk.at[pl.ds(pl.multiple_of(n * rows, rows), rows), pl.ds(i * dt, dt)]

    def a_copy(n, hf):
        return remote(out.at[n, pl.ds(hf * hr, hr)], land(n, 2).at[pl.ds(hf * hr, hr)], a_s.at[n, hf], a_r.at[n, hf], (fp, fm)[hf])

    def b_copy(n, i):
        return remote(out.at[n, pl.ds((1 + i) * rows, rows)], land(n, i), b_s.at[n, i], b_r.at[n, i], (fp, fm)[i])

    def y_copy(n):
        cols = pl.ds(pl.multiple_of(n * dt, dt), dt)
        return pltpu.make_async_copy(out.at[n, pl.ds(3 * rows, rows)], y.at[:, cols], ysem.at[n])

    def rounds(xb):
        start(u_copies(0, 0))
        start(u_part(1, 0, 1))
        for i in range(2):
            load_small(xb, 0, i, 0, 0, i)
        barrier = pltpu.get_barrier_semaphore()
        for dev in (fp, fm, sp, sm, sib):
            pl.semaphore_signal(barrier, 1, device_id={"tp": dev})
        pl.semaphore_wait(barrier, 5)

        for hf in range(2):
            hand(0, 0, hf).start()
        for hf in range(2):
            move(source(0, 0, hf), 0, 1, hf, fp).start()
            move(source(0, 0, hf), 0, 2, hf, fm).start()
        inb[...] = jnp.zeros_like(inb)
        for i in range(2, 4):
            load_small(xb, 0, i, 0, 0, i - 2)

        def on(i, v, *calls):
            @when(i == v)
            def _():
                for fn, *a in calls:
                    fn(*a)

        def hook(i):
            on(i, nt - 2, (arrive, 0, 1, 0), (arrive, 0, 2, 0), (load_mid, xb, 1, 0))

        u_small(xb, 0, (0, hr), (row0(0, 0), row0(0, 1)), 0, hook, True, 1)
        arrive(0, 1, 1)
        arrive(0, 2, 1)
        forward(0, 0)
        forward(0, 1)
        for i in range(1, 4):
            load_mid(xb, 1, i)

        def hook(i):
            @when(i < pieces // 3)
            def _():
                w_piece(i).start()

            on(i, 3, (push, 1, 0))
            on(i, 4, (forward, 0, 2))
            on(i, 5, (push, 1, 1), (load_pair, xb, 0, 0, 0, 1, 0, 0), (load_pair, xb, 0, 1, 0, 1, 0, 1))

        u_big(xb, 1, (seg, half_rows + seg), (row0(1, 0), row0(1, 1)), 1, hook)
        for hf in range(2):
            load_pair(xb, 0, 2 + hf, 1, 1, 0, hf)

        def one_round(k, carry):
            fi = 2 // (k + 1)
            first = k == 1

            def up(it, carry):
                b = fi * (it // nt) + (1 - fi) * lax.rem(it, 2)
                i = fi * lax.rem(it, nt) + (1 - fi) * (it // 2)
                ws = lax.rem(i, 2)

                @when(first)
                def _():
                    @when(it < pieces // 3)
                    def _():
                        w_piece(pieces // 3 + it).start()

                    @when((it > nt) & (it <= nt + pieces // 3))
                    def _():
                        w_piece(2 * (pieces // 3) + it - nt - 1).start()

                    def keep(c):
                        return (c * seg, half_rows + c * seg)

                    def where(c):
                        return (row0(2 * c, 0), row0(2 * c, 1))

                    on(it, 0, (h_sent, 0, hr))
                    on(it, 0, (far, 1, 0))
                    on(it, 1, (push, 1, 2), (far, 1, 1))
                    on(it, 4, (push, 1, 3), (forward, 1, 0))
                    on(it, 5, (load_pair, xb, 1, 0, 0, 1, 1, 0), (load_pair, xb, 1, 1, 0, 1, 1, 1),
                       (load_pair, xb, 1, 2, 1, 1, 1, 0), (load_pair, xb, 1, 3, 1, 1, 1, 1))
                    on(it, nt, (h_push, hk, 3, parts - 1, keep(0), where(0), seg), (h_sent, 1, seg), (forward, 1, 1))
                    on(it, 7, (forward, 1, 2))
                    on(it, 8, (forward, 1, 3))
                    on(it, 9, (push, 2, 0))
                    on(it, 11, (push, 2, 1))
                    for part in range(parts - 1):
                        for c in range(2):
                            on(it, c * nt + cuts[part + 1], (h_push, hk, 3 + c, part, keep(c), where(c), seg))

                @when(k > 1)
                def _():
                    on(it, 2 * nt - 2, (in_start, k - 2, 0))
                    for part in range(1, parts):
                        @when(it == 2 * nt - 3 + part)
                        def _():
                            hy_copy(part).start()

                @when(first & (it < 2 * nt - 1))
                def _():
                    start(u_copies(lax.rem(i + 1, nt), 1 - ws))

                @when(it == 2 * nt - 1)
                def _():
                    @when(first)
                    def _():
                        for q in range(pieces):
                            w_piece(q).wait_recv()

                    start(d_copies(0, 0))

                @when(first & (i == 0))
                def _():
                    loaded(xb, b, seg)

                @when(first | (b == 0))
                def _():
                    wait(u_copies(i, ws))

                h = hidden(xb.at[b], ws)
                for q in range(4):
                    r = fi * (q * half_rows + b * seg) + (1 - fi) * ((1 - b) * m + q * seg)
                    hk[pl.ds(pl.multiple_of(r, seg), seg), u_cols(i)] = h[q * seg : (q + 1) * seg]
                return carry

            def up_both(i, carry):
                ws = lax.rem(i, 2)
                start(u_copies(i + 1, 1 - ws))

                @when(k == 2)
                def _():
                    on(i, 0, (h_sent, 3, seg), (h_sent, 4, seg))
                    on(i, 2, (push, 3, 0))
                    on(i, 4, (push, 3, 1))

                @when(k == 3)
                def _():
                    on(i, 4, (push, 0, 3))

                    @when(i == 0)
                    def _():
                        for part in range(parts):
                            hy_copy(part).wait_send()

                @when(i == cuts[1])
                def _():
                    pl.semaphore_wait(hfree, 1)
                    hy_copy(0).start()

                @when(i == 0)
                def _():
                    for slot in range(2):
                        loaded(xb, slot, seg)

                wait(u_copies(i, ws))
                hk[pl.ds(m, m), u_cols(i)] = hidden(xb.at[0], ws)
                hk[pl.ds(0, m), u_cols(i)] = hidden(xb.at[1], ws)
                return carry

            lax.fori_loop(0, (1 - fi) * (nt - 1), up_both, 0)
            lax.fori_loop((1 - fi) * 2 * (nt - 1), 2 * nt, up, 0)

            @when(first)
            def _():
                h_push(hk, 4, parts - 1, (seg, half_rows + seg), (row0(2, 0), row0(2, 1)), seg)
                h_here(3, seg)
                h_here(4, seg)

            @when(k > 1)
            def _():
                for part in range(parts):
                    hy_copy(part).wait_recv()

            def down(n, carry):
                ws = lax.rem(n, 2)

                @when(n < nd - 1)
                def _():
                    start(d_copies(n + 1, 1 - ws))

                @when(n == nd - 1)
                def _():
                    start(u_copies(0, 0))

                @when(k > 1)
                def _():
                    in_copy(k - 2, n).wait()

                    @when(n < nd - 1)
                    def _():
                        in_start(k - 2, n + 1)

                    for hf in range(2):
                        sum_copy(0, n, hf).wait_send()

                @when(first)
                def _():
                    on(n, 0, (forward, 2, 0))
                    on(n, 1, (push, 2, 2))
                    on(n, 2, (forward, 2, 1))
                    on(n, 4, (push, 2, 3))
                    on(n, 5, (forward, 2, 2))
                    on(n, 7, (forward, 2, 3))

                @when(k == 2)
                def _():
                    on(n, 2, (push, 3, 2))
                    on(n, 4, (push, 3, 3))
                    on(n, 7, (far, 0, 0), (far, 0, 1))

                @when(k < 3)
                def _():
                    for v, other, pair in ((1, 0, 0), (3, 1, 0), (5, 0, 1), (6, 1, 1)):
                        @when(n == v)
                        def _():
                            for hf in range(2):
                                load_pair(xb, 1 - other, 2 * hf + pair, other, k + 1, pair, hf)

                @when(k == 3)
                def _():
                    for q in range(4):
                        on(n, 2 + q, (load_small, xb, 0, q, 0, 3, q % 2))

                wait(d_copies(n, ws))
                for q in range(sub):
                    total, cols = products(hk.at[pl.ds(0, m)], n, q)
                    out[n, :, cols] = total.astype(BF16)
                for hf in range(2):
                    sum_copy(k - 1, n, hf).start()
                return carry

            lax.fori_loop(0, nd, down, 0)

            @when(k < 3)
            def _():
                pl.semaphore_signal(hfree, 1, device_id={"tp": sib})

            return carry

        lax.fori_loop(1, side, one_round, 0)

        def hook(i):
            on(i, nt - 2, (in_start, 2, 0))

        for part in range(parts):
            hy_copy(part).wait_send()
        u_small(xb, 0, (0, hr), (row0(3, 0), row0(3, 1)), 5, hook, False, 0)

    pl.run_scoped(rounds, pltpu.VMEM((2, 8 * hr, d), BF16))

    def last(t0, t1, t2):
        h_sent(5, hr)
        for dev in (fp, fm):
            pl.semaphore_signal(nfree, 1, device_id={"tp": dev})
        for idx, size in ((0, hr), (1, seg), (5, hr)):
            h_here(idx, size)

        def add_far(n):
            for hf in range(2):
                a_copy(n, hf).wait_recv()
            far_in = land(n, 2)[...].astype(F32)
            out[n, pl.ds(rows, hr)] = (t2[n, :hr] + far_in[:hr]).astype(BF16)
            out[n, pl.ds(rows + hr, hr)] = t2[n, hr:].astype(BF16)
            out[n, pl.ds(2 * rows, hr)] = t1[n, :hr].astype(BF16)
            out[n, pl.ds(2 * rows + hr, hr)] = (t1[n, hr:] + far_in[hr:]).astype(BF16)
            for i in range(2):
                b_copy(n, i).start()

        def add_near(n):
            for i in range(2):
                b_copy(n, i).wait_recv()
            out[n, pl.ds(3 * rows, rows)] = (t0[n] + land(n, 0)[...].astype(F32) + land(n, 1)[...].astype(F32)).astype(BF16)
            y_copy(n).start()

        def down(n, carry):
            ws = lax.rem(n, 2)

            @when(n < nd - 1)
            def _():
                start(d_copies(n + 1, 1 - ws))

            in_copy(2, n).wait()

            @when(n < nd - 1)
            def _():
                in_start(2, n + 1)

            for hf in range(2):
                sum_copy(0, n, hf).wait_send()

            @when(n >= 2)
            def _():
                add_far(n - 2)

            @when(n >= 4)
            def _():
                add_near(n - 4)

            wait(d_copies(n, ws))
            for q in range(sub):
                total, cols = products(h0, n, q)
                for hf in range(2):
                    o = hf * half_rows
                    dst = pl.ds(hf * hr, hr)
                    t0[n, dst, cols] = total[o : o + hr]
                    t1[n, dst, cols] = total[o + hr : o + 2 * hr]
                    t2[n, dst, cols] = total[o + 2 * hr : o + 3 * hr]
                    out[n, dst, cols] = total[o + 3 * hr : o + 4 * hr].astype(BF16)
            @when(n == 0)
            def _():
                pl.semaphore_wait(nfree, 2)

            for hf in range(2):
                a_copy(n, hf).start()
            return carry

        lax.fori_loop(0, nd, down, 0)
        add_far(nd - 2)
        add_near(nd - 4)
        add_far(nd - 1)
        for n in range(nd - 3, nd):
            add_near(n)

    shape = pltpu.VMEM((nd, rows, dt), F32)
    pl.run_scoped(last, shape, shape, shape)

    for n in range(nd):
        y_copy(n).wait()
        for i in range(2):
            a_copy(n, i).wait_send()
            b_copy(n, i).wait_send()
    for i in range(pieces):
        w_piece(i).wait_send()
    for k in range(side):
        for j in range(side):
            for hf in range(2):
                hand(k, j, hf).wait_send()
                if k or j:
                    move(piece(k, j, hf), k, j, hf, sib).wait_send()


def build(mesh, tn, dt):
    side = math.isqrt(mesh.shape["tp"] // 2)

    def step(x, w_gate, w_up, w_down):
        rows, d = x.shape
        hid = w_gate.shape[1]
        hr = rows // 2
        nt, nd = hid // tn, d // dt
        dma = pltpu.SemaphoreType.DMA
        hbm = pl.BlockSpec(memory_space=pltpu.HBM)
        m = side * rows
        result = pl.pallas_call(
            functools.partial(kernel, side, tn, dt),
            out_shape=(
                jax.ShapeDtypeStruct((rows, d), BF16),
                jax.ShapeDtypeStruct((2, side, m, d), BF16),
                jax.ShapeDtypeStruct((hid, d), BF16),
                jax.ShapeDtypeStruct((side - 1, nd, m, dt), BF16),
            ),
            in_specs=[hbm] * 4,
            out_specs=[hbm] * 4,
            scratch_shapes=[
                pltpu.VMEM((2, 2, d, tn), BF16),
                pltpu.VMEM((m, 2 * hid), BF16),
                pltpu.VMEM((2 * m, 2 * hid), BF16),
                pltpu.VMEM((nd, m, dt), BF16),
                pltpu.VMEM((2, m, dt), BF16),
                dma((2, 2 * dt // tn)),
                dma((2, 4)),
                dma((2,)),
                dma((nd,)),
                dma((side, 2 * side)),
                dma((side, 2 * side)),
                dma((side, 2 * side)),
                dma((side, 2 * side)),
                dma((12,)),
                dma((12,)),
                dma((6, 6)),
                dma((6, 6)),
                dma((3,)),
                dma((3,)),
                dma((nd, 2)),
                dma((side - 1, 2 * nd)),
                dma((nd, 2)),
                dma((nd, 2)),
                dma((nd, 2)),
                dma((nd, 2)),
                pltpu.SemaphoreType.REGULAR,
                pltpu.SemaphoreType.REGULAR,
            ],
            compiler_params=pltpu.CompilerParams(collective_id=0, has_side_effects=True, vmem_limit_bytes=67043328),
            cost_estimate=pl.CostEstimate(flops=6 * side * side * 2 * rows * d * hid, bytes_accessed=9 * d * hid * 4, transcendentals=0),
            name="mlp",
        )(x, w_gate, w_up, w_down)
        return result[0]

    return jax.shard_map(
        step,
        mesh=mesh,
        in_specs=(P(("dp", "tp"), None), P(None, "tp"), P(None, "tp"), P("tp", None)),
        out_specs=P(("dp", "tp"), None),
        check_vma=False,
    )


def solution(mesh):
    return build(mesh, 256, 1024)
```

```python
import functools
import math

import jax
import jax.numpy as jnp
from jax import lax
from jax.experimental import pallas as pl
from jax.experimental.pallas import tpu as pltpu
from jax.sharding import PartitionSpec as P

F32, BF16 = jnp.float32, jnp.bfloat16


def kernel(side, tn, dt, x, wg, wu, wd, y, xs, wp, rs, wbuf, h0, hk, out, inb, wsem, xsem, isem, ysem,
           ag_s, ag_r, pu_s, pu_r, wp_s, wp_r, hx_s, hx_r, hy_s, hy_r, rs_s, rs_r, a_s, a_r, b_s, b_r, hfree, nfree):
    rows, d = x.shape
    hid = wg.shape[1]
    hr = rows // 2
    half_rows = side * hr
    m = 2 * half_rows
    seg = 2 * hr
    nt, nd = hid // tn, d // dt
    sub = dt // tn
    cuts = (0, nt // 3, nt - 1, nt)
    parts = len(cuts) - 1
    pieces = 2 * nt
    dt2, ne = dt // 2, 2 * nd

    t = lax.axis_index("tp")
    c = lax.rem(t, 2)
    cx, cy = t // (2 * side), lax.rem(t // 2, side)
    f, s = cx * (1 - c) + cy * c, cy * (1 - c) + cx * c

    def at(df, ds):
        ff, ss = lax.rem(f + df + side, side), lax.rem(s + ds + side, side)
        return ((ff * (1 - c) + ss * c) * side + ss * (1 - c) + ff * c) * 2 + c

    fp, fm, sp, sm, sib = at(1, 0), at(-1, 0), at(0, 1), at(0, -1), t + 1 - 2 * c

    def remote(src, dst, send, recv, dev):
        return pltpu.make_async_remote_copy(src_ref=src, dst_ref=dst, send_sem=send, recv_sem=recv, device_id={"tp": dev})

    def when(cond):
        return pl.when(cond)

    def row0(j, hf):
        return hf * half_rows + j * hr

    def piece(k, j, hf, other=0):
        return xs.at[other, k, pl.ds(row0(j, hf), hr)]

    def source(k, j, hf):
        if isinstance(k, int) and isinstance(j, int) and k == 0 and j == 0:
            return x.at[pl.ds(hf * hr, hr)]
        return piece(k, j, hf)

    def move(src, k, j, hf, dev):
        i = j * 2 + hf
        return remote(src, piece(k, j, hf), ag_s, ag_r.at[k, i], dev)

    def hand(k, j, hf):
        i = j * 2 + hf
        return remote(source(k, j, hf), piece(k, j, hf, 1), pu_s, pu_r.at[k, i], sib)

    def arrive(k, j, hf):
        move(piece(k, j, hf), k, j, hf, sib).wait_recv()
        hand(k, j, hf).start()

    def push(k, j):
        for hf in range(2):
            arrive(k, j, hf)

    def forward(k, j):
        for hf, dev in ((0, sp), (1, sm)):
            move(source(k, j, hf), k + 1, j, hf, dev).start()

    def far(k, hf):
        move(piece(k, 1 + hf, hf), k, 3, hf, (fp, fm)[hf]).start()

    def load(xb, slot, row, src, size, sem):
        pltpu.make_async_copy(src, xb.at[slot, pl.ds(row, size)], xsem.at[sem]).start()

    def loaded(xb, slot, row, size, sem):
        dst = xb.at[slot, pl.ds(row, size)]
        pltpu.make_async_copy(dst, dst, xsem.at[sem]).wait()

    def load_small(xb, i, k, j, hf):
        if i < 2:
            src = source(k, j, hf)
        else:
            hand(k, j, hf).wait_recv()
            src = piece(k, j, hf, 1)
        load(xb, 0, i * hr, src, hr, 0)

    def load_mid(xb, other, hf):
        if other:
            for j in (1, 2):
                hand(0, j, hf).wait_recv()
        load(xb, 1, (2 * hf + other) * seg, xs.at[other, 0, pl.ds(row0(1, hf), seg)], seg, 1 + hf)

    def load_pair(xb, slot, i, other, k, pair, hf):
        for q in range(2):
            @when(other == 1)
            def _():
                hand(k, 2 * pair + q, hf).wait_recv()
        load(xb, slot, i * seg, xs.at[other, k, pl.ds(hf * half_rows + pair * seg, seg)], seg, slot)

    def u_part(n, z, slot):
        cols, depth = pl.ds(pl.multiple_of(n * tn, tn), tn), pl.ds(z * (d // 2), d // 2)
        return [pltpu.make_async_copy(w.at[depth, cols], wbuf.at[slot, i, depth], wsem.at[slot, z]) for i, w in enumerate((wg, wu))]

    def u_copies(n, slot):
        return u_part(n, 0, slot) + u_part(n, 1, slot)

    def d_rows(q):
        return q // 2, (q % 2) * 2 * hid

    def d_copies(n, slot):
        r = []
        for q in range(sub):
            p, o = d_rows(q)
            cols = pl.ds(pl.multiple_of(n * dt + q * tn, tn), tn)
            for i, w in enumerate((wd, wp)):
                r.append(pltpu.make_async_copy(w.at[:, cols], wbuf.at[slot, p, pl.ds(o + i * hid, hid)], wsem.at[slot, 0]))
        return r

    def start(copies):
        for cp in copies:
            cp.start()

    def held(slot, z, depth):
        dst = wbuf.at[slot, :, depth]
        pltpu.make_async_copy(dst, dst, wsem.at[slot, z]).wait()

    def u_held(z, slot):
        held(slot, z, pl.ds(z * (d // 2), d // 2))

    def d_held(slot):
        held(slot, 0, pl.ds(0, sub * hid))

    def cut(part):
        return cuts[part] * tn, (cuts[part + 1] - cuts[part]) * tn

    def h_copy(hdst, idx, part, src, dst, size):
        lo, width = cut(part)
        return remote(hk.at[pl.ds(m + src, size), pl.ds(lo, width)], hdst.at[pl.ds(dst, size), pl.ds(hid + lo, width)],
                      hx_s.at[idx], hx_r.at[idx], sib)

    def h_push(hdst, idx, part, src, dst, size):
        for q in range(2):
            h_copy(hdst, idx, part, src[q], dst[q], size).start()

    def h_all(idx, size):
        r = pl.ds(0, 2 * size)
        return remote(hk.at[r, pl.ds(0, hid)], hk.at[r, pl.ds(hid, hid)], hx_s.at[idx], hx_r.at[idx], sib)

    def h_sent(idx, size):
        h_all(idx, size).wait_send()

    def h_here(idx, size):
        h_all(idx, size).wait_recv()

    def hy_copy(lo, size):
        return remote(hk.at[pl.ds(m, m), pl.ds(lo, size)], hk.at[pl.ds(0, m), pl.ds(hid + lo, size)], hy_s, hy_r, sib)

    def hy_all():
        return hy_copy(0, hid)

    def w_piece(i):
        r = pl.ds(i * (hid // pieces), hid // pieces)
        return remote(wd.at[r], wp.at[r], wp_s, wp_r, sib)

    def hidden(lhs, ws):
        gate = jnp.dot(lhs[...], wbuf[ws, 0], preferred_element_type=F32)
        up = jnp.dot(lhs[...], wbuf[ws, 1], preferred_element_type=F32)
        return (jax.nn.silu(gate) * up).astype(BF16)

    def u_cols(i):
        return pl.ds(pl.multiple_of(i * tn, tn), tn)

    def u_small(xb, slot, row, sem, keep, where, idx, hook, end, ahead, nxt):
        half = d // 2

        def after(i, more):
            return lax.rem(i + more, end) if nxt == 2 else i + more

        def body(i, carry):
            ws = lax.rem(i, 2)
            hook(i)

            for part in range(parts):
                if cuts[part + 1] < end:
                    @when(i == cuts[part + 1])
                    def _():
                        h_push(h0, idx, part, keep, where, hr)

            if not ahead:
                @when(i == 0)
                def _():
                    start(u_part(1, 0, 1))

            if nxt:
                start(u_part(after(i, 1), 1, 1 - ws))
            else:
                @when(i < end - 1)
                def _():
                    start(u_part(i + 1, 1, 1 - ws))

                @when(i == end - 1)
                def _():
                    start(d_copies(0, 0))

            @when(i == 0)
            def _():
                loaded(xb, slot, row, 4 * hr, sem)

            def products_of(z):
                u_held(z, ws)
                depth = pl.ds(z * half, half)
                lhs = xb[slot, pl.ds(row, 4 * hr), depth]
                return [jnp.dot(lhs, wbuf[ws, q, depth], preferred_element_type=F32) for q in range(2)]

            gate, up = products_of(0)

            if nxt == 2:
                start(u_part(after(i, 2), 0, ws))
            else:
                @when(i < end - 2 + nxt)
                def _():
                    start(u_part(i + 2, 0, ws))

            gate2, up2 = products_of(1)
            h = (jax.nn.silu(gate + gate2) * (up + up2)).astype(BF16)
            for q in range(2):
                h0[pl.ds(where[q], hr), u_cols(i)] = h[q * hr : (q + 1) * hr]
                hk[pl.ds(m + keep[q], hr), u_cols(i)] = h[(2 + q) * hr : (3 + q) * hr]
            return carry

        lax.fori_loop(0, end, body, 0)
        for part in range(parts):
            if cuts[part + 1] == end:
                h_push(h0, idx, part, keep, where, hr)

    def u_big(xb, keep, where, idx, hook, begin):
        def body(i, carry):
            ws = lax.rem(i, 2)
            hook(i)

            for part in range(1, parts - 1):
                @when(i == cuts[part + 1])
                def _():
                    h_push(h0, idx, part, keep, where, seg)

            start(u_copies(lax.rem(i + 1, nt), 1 - ws))
            u_held(0, ws)
            u_held(1, ws)
            h = hidden(xb.at[1], ws)
            for q in range(2):
                h0[pl.ds(where[q], seg), u_cols(i)] = h[2 * q * seg : (2 * q + 1) * seg]
                hk[pl.ds(m + keep[q], seg), u_cols(i)] = h[(2 * q + 1) * seg : (2 * q + 2) * seg]
            return carry

        lax.fori_loop(begin, nt, body, 0)
        h_push(h0, idx, parts - 1, keep, where, seg)

    def sum_copy(hop, n, hf):
        part = pl.ds(hf * half_rows, half_rows)
        return remote(out.at[n, part], rs.at[hop, n, part], rs_s.at[n], rs_r.at[hop, n], (sp, sm)[hf])

    def sum_all(hop, n):
        return remote(out.at[n], rs.at[hop, n], rs_s.at[n], rs_r.at[hop, n], sp)

    def in_copy(hop, n):
        b = lax.rem(n, 2)
        return pltpu.make_async_copy(rs.at[hop, n], inb.at[b], isem.at[b])

    def in_start(hop, n):
        sum_all(hop, n).wait_recv()
        in_copy(hop, n).start()

    def products(h, n, q):
        p, o = d_rows(q)
        ws = lax.rem(n, 2)
        cols = slice(q * tn, (q + 1) * tn)
        term = jnp.dot(h[...], wbuf[ws, p, pl.ds(o, 2 * hid)], preferred_element_type=F32)
        return term + inb[lax.rem(n, 2), :, cols].astype(F32), cols

    def step_cols(e, base=0):
        return pl.ds(pl.multiple_of(base + lax.rem(e, 2) * dt2, dt2), dt2)

    def land(e, i):
        r = pl.ds(pl.multiple_of((e // 2) * rows, rows), rows)
        return hk.at[r, step_cols(e, i * dt)]

    def leave(e, row, size):
        return out.at[e // 2, pl.ds(row, size), step_cols(e)]

    def a_copy(e, hf):
        return remote(leave(e, hf * hr, hr), land(e, 2).at[pl.ds(hf * hr, hr)], a_s, a_r.at[e], (fp, fm)[hf])

    def b_copy(e, i):
        return remote(leave(e, (1 + i) * rows, rows), land(e, i), b_s, b_r.at[e], (fp, fm)[i])

    def y_copy(e):
        cols = pl.ds(pl.multiple_of(e * dt2, dt2), dt2)
        return pltpu.make_async_copy(leave(e, 3 * rows, rows), y.at[:, cols], ysem)

    def rounds(xb):
        start(u_copies(0, 0))
        start(u_part(1, 0, 1))
        for i in range(2):
            load_small(xb, i, 0, 0, i)
        barrier = pltpu.get_barrier_semaphore()
        for dev in (fp, fm, sp, sm, sib):
            pl.semaphore_signal(barrier, 1, device_id={"tp": dev})
        pl.semaphore_wait(barrier, 5)

        for hf in range(2):
            hand(0, 0, hf).start()
        for hf in range(2):
            move(source(0, 0, hf), 0, 1, hf, fp).start()
            move(source(0, 0, hf), 0, 2, hf, fm).start()
        inb[...] = jnp.zeros_like(inb)
        for i in range(2, 4):
            load_small(xb, i, 0, 0, i - 2)

        def on(i, v, *calls):
            @when(i == v)
            def _():
                for fn, *a in calls:
                    fn(*a)

        def hook(i):
            on(i, nt - 3, (arrive, 0, 1, 0), (arrive, 0, 2, 0), (load_mid, xb, 0, 0))
            on(i, nt - 1, (load_mid, xb, 1, 0))

        u_small(xb, 0, 0, 0, (0, hr), (row0(0, 0), row0(0, 1)), 0, hook, nt, True, 2)

        def hook(i):
            on(i, 0, (forward, 0, 0))
            on(i, 1, (arrive, 0, 1, 1), (arrive, 0, 2, 1), (forward, 0, 1), (load_mid, xb, 0, 1))

        u_small(xb, 1, 0, 1, (seg, seg + hr), (row0(1, 0), row0(2, 0)), 1, hook, cuts[1], True, 2)
        load_mid(xb, 1, 1)

        def hook(i):
            pass

        u_small(xb, 1, 2 * seg, 2, (half_rows + seg, half_rows + seg + hr), (row0(1, 1), row0(2, 1)), 1, hook, cuts[1], True, 1)

        def hook(i):
            @when(i < cuts[1] + 2)
            def _():
                for q in range(2):
                    w_piece(2 * (i - cuts[1]) + q).start()

            on(i, nt - 2, (forward, 0, 2), (push, 1, 0))
            on(i, nt - 1, (push, 1, 1), (load_pair, xb, 0, 0, 0, 1, 0, 0), (load_pair, xb, 0, 1, 0, 1, 0, 1))

        u_big(xb, (seg, half_rows + seg), (row0(1, 0), row0(1, 1)), 1, hook, cuts[1])
        for hf in range(2):
            load_pair(xb, 0, 2 + hf, 1, 1, 0, hf)

        def one_round(k, carry):
            fi = 2 // (k + 1)
            first = k == 1

            def up(it, carry):
                b = fi * (it // nt) + (1 - fi) * lax.rem(it, 2)
                i = fi * lax.rem(it, nt) + (1 - fi) * (it // 2)
                ws = lax.rem(i, 2)

                @when(first)
                def _():
                    @when(it < pieces // 3)
                    def _():
                        w_piece(pieces // 3 + it).start()

                    @when((it > nt) & (it <= nt + pieces // 3))
                    def _():
                        w_piece(2 * (pieces // 3) + it - nt - 1).start()

                    def keep(c):
                        return (c * seg, half_rows + c * seg)

                    def where(c):
                        return (row0(2 * c, 0), row0(2 * c, 1))

                    on(it, 0, (h_sent, 0, hr))
                    on(it, 0, (far, 1, 0))
                    on(it, 1, (push, 1, 2), (far, 1, 1))
                    on(it, 4, (push, 1, 3), (forward, 1, 0))
                    on(it, 5, (load_pair, xb, 1, 0, 0, 1, 1, 0), (load_pair, xb, 1, 1, 0, 1, 1, 1),
                       (load_pair, xb, 1, 2, 1, 1, 1, 0), (load_pair, xb, 1, 3, 1, 1, 1, 1))
                    on(it, nt, (h_push, hk, 3, parts - 1, keep(0), where(0), seg), (h_sent, 1, seg), (forward, 1, 1))
                    on(it, 7, (forward, 1, 2))
                    on(it, 8, (forward, 1, 3))
                    on(it, 9, (push, 2, 0))
                    on(it, 11, (push, 2, 1))
                    for part in range(parts - 1):
                        for c in range(2):
                            on(it, c * nt + cuts[part + 1], (h_push, hk, 3 + c, part, keep(c), where(c), seg))

                @when(k > 1)
                def _():
                    on(it, 2 * nt - 2, (in_start, k - 2, 0))
                    for part in range(1, parts):
                        @when(it == 2 * nt - 3 + part)
                        def _():
                            hy_copy(*cut(part)).start()

                @when(first & (it < 2 * nt - 1))
                def _():
                    start(u_copies(lax.rem(i + 1, nt), 1 - ws))

                @when(it == 2 * nt - 1)
                def _():
                    @when(first)
                    def _():
                        remote(wd, wp, wp_s, wp_r, sib).wait_recv()

                    start(d_copies(0, 0))

                @when(first & (i == 0))
                def _():
                    loaded(xb, b, 0, 4 * seg, b)

                @when(first | (b == 0))
                def _():
                    u_held(0, ws)
                    u_held(1, ws)

                h = hidden(xb.at[b], ws)
                for q in range(4):
                    r = fi * (q * half_rows + b * seg) + (1 - fi) * ((1 - b) * m + q * seg)
                    hk[pl.ds(pl.multiple_of(r, seg), seg), u_cols(i)] = h[q * seg : (q + 1) * seg]
                return carry

            def up_both(i, carry):
                ws = lax.rem(i, 2)
                start(u_copies(i + 1, 1 - ws))

                @when(k == 2)
                def _():
                    on(i, 0, (h_sent, 3, seg), (h_sent, 4, seg))
                    on(i, 2, (push, 3, 0))
                    on(i, 4, (push, 3, 1))

                @when(k == 3)
                def _():
                    on(i, 4, (push, 0, 3))

                    @when(i == 0)
                    def _():
                        hy_all().wait_send()

                @when(i == cuts[1])
                def _():
                    pl.semaphore_wait(hfree, 1)
                    hy_copy(*cut(0)).start()

                @when(i == 0)
                def _():
                    for slot in range(2):
                        loaded(xb, slot, 0, 4 * seg, slot)

                u_held(0, ws)
                u_held(1, ws)
                hk[pl.ds(m, m), u_cols(i)] = hidden(xb.at[0], ws)
                hk[pl.ds(0, m), u_cols(i)] = hidden(xb.at[1], ws)
                return carry

            lax.fori_loop(0, (1 - fi) * (nt - 1), up_both, 0)
            lax.fori_loop((1 - fi) * 2 * (nt - 1), 2 * nt, up, 0)

            @when(first)
            def _():
                h_push(hk, 4, parts - 1, (seg, half_rows + seg), (row0(2, 0), row0(2, 1)), seg)
                h_here(3, seg)
                h_here(4, seg)

            @when(k > 1)
            def _():
                hy_all().wait_recv()

            def down(n, carry):
                ws = lax.rem(n, 2)

                @when(n < nd - 1)
                def _():
                    start(d_copies(n + 1, 1 - ws))

                @when(n == nd - 1)
                def _():
                    start(u_copies(0, 0))

                @when(k > 1)
                def _():
                    in_copy(k - 2, n).wait()

                    @when(n < nd - 1)
                    def _():
                        in_start(k - 2, n + 1)

                    sum_all(0, n).wait_send()

                @when(first)
                def _():
                    on(n, 0, (forward, 2, 0))
                    on(n, 1, (push, 2, 2))
                    on(n, 2, (forward, 2, 1))
                    on(n, 4, (push, 2, 3))
                    on(n, 5, (forward, 2, 2))
                    on(n, 7, (forward, 2, 3))

                @when(k == 2)
                def _():
                    on(n, 2, (push, 3, 2))
                    on(n, 4, (push, 3, 3))
                    on(n, 7, (far, 0, 0), (far, 0, 1))

                @when(k < 3)
                def _():
                    for v, other, pair in ((1, 0, 0), (3, 1, 0), (5, 0, 1), (6, 1, 1)):
                        @when(n == v)
                        def _():
                            for hf in range(2):
                                load_pair(xb, 1 - other, 2 * hf + pair, other, k + 1, pair, hf)

                @when(k == 3)
                def _():
                    for q in range(4):
                        on(n, 2 + q, (load_small, xb, q, 0, 3, q % 2))

                d_held(ws)
                for q in range(sub):
                    total, cols = products(hk.at[pl.ds(0, m)], n, q)
                    out[n, :, cols] = total.astype(BF16)
                for hf in range(2):
                    sum_copy(k - 1, n, hf).start()
                return carry

            lax.fori_loop(0, nd, down, 0)

            @when(k < 3)
            def _():
                pl.semaphore_signal(hfree, 1, device_id={"tp": sib})

            return carry

        lax.fori_loop(1, side, one_round, 0)

        def hook(i):
            on(i, nt - 2, (in_start, 2, 0))

        hy_all().wait_send()
        u_small(xb, 0, 0, 0, (0, hr), (row0(3, 0), row0(3, 1)), 5, hook, nt, False, 0)

    pl.run_scoped(rounds, pltpu.VMEM((2, 8 * hr, d), BF16))

    def last(t0, t1, t2):
        h_sent(5, hr)
        for dev in (fp, fm):
            pl.semaphore_signal(nfree, 1, device_id={"tp": dev})
        for idx, size in ((0, hr), (1, seg), (5, hr)):
            h_here(idx, size)

        def add_far(e):
            both = pl.ds(0, rows)
            remote(out.at[0, both, pl.ds(0, dt2)], land(e, 2), a_s, a_r.at[e], fp).wait_recv()
            far_in = land(e, 2)[...].astype(F32)
            leave(e, rows, hr)[...] = (t2[e, :hr] + far_in[:hr]).astype(BF16)
            leave(e, rows + hr, hr)[...] = t2[e, hr:].astype(BF16)
            leave(e, 2 * rows, hr)[...] = t1[e, :hr].astype(BF16)
            leave(e, 2 * rows + hr, hr)[...] = (t1[e, hr:] + far_in[hr:]).astype(BF16)
            for i in range(2):
                b_copy(e, i).start()

        def add_near(e):
            both = pl.ds(0, 2 * rows)
            remote(out.at[0, both, pl.ds(0, dt2)], out.at[0, both, pl.ds(0, dt2)], b_s, b_r.at[e], fp).wait_recv()
            leave(e, 3 * rows, rows)[...] = (t0[e] + land(e, 0)[...].astype(F32) + land(e, 1)[...].astype(F32)).astype(BF16)
            y_copy(e).start()

        def down(e, carry):
            n, c2 = e // 2, lax.rem(e, 2)
            ws = lax.rem(n, 2)

            @when(c2 == 0)
            def _():
                @when(n < nd - 1)
                def _():
                    start(d_copies(n + 1, 1 - ws))

                in_copy(2, n).wait()

                @when(n < nd - 1)
                def _():
                    in_start(2, n + 1)

                sum_all(0, n).wait_send()
                d_held(ws)

            @when(e >= 3)
            def _():
                add_far(e - 3)

            @when(e >= 6)
            def _():
                add_near(e - 6)

            for q in range(2):
                term = jnp.dot(h0[...], wbuf[ws, c2, pl.ds(q * 2 * hid, 2 * hid)], preferred_element_type=F32)
                cols = slice(q * tn, (q + 1) * tn)
                total = term + inb[lax.rem(n, 2), :, pl.ds(pl.multiple_of(c2 * dt2 + q * tn, tn), tn)].astype(F32)
                for hf in range(2):
                    o = hf * half_rows
                    dst = pl.ds(hf * hr, hr)
                    t0[e, dst, cols] = total[o : o + hr]
                    t1[e, dst, cols] = total[o + hr : o + 2 * hr]
                    t2[e, dst, cols] = total[o + 2 * hr : o + 3 * hr]
                    out[n, dst, pl.ds(pl.multiple_of(c2 * dt2 + q * tn, tn), tn)] = total[o + 3 * hr : o + 4 * hr].astype(BF16)

            @when(e == 0)
            def _():
                pl.semaphore_wait(nfree, 2)

            for hf in range(2):
                a_copy(e, hf).start()
            return carry

        lax.fori_loop(0, ne, down, 0)
        for i in range(3):
            add_near(ne - 6 + i)
            add_far(ne - 3 + i)
        for i in range(3):
            add_near(ne - 3 + i)

    shape = pltpu.VMEM((ne, rows, dt2), F32)
    pl.run_scoped(last, shape, shape, shape)

    pltpu.make_async_copy(y, y, ysem).wait()
    for sem, r in ((a_s, pl.ds(0, rows)), (b_s, pl.ds(rows, 2 * rows))):
        remote(out.at[:, r], out.at[:, r], sem, a_r.at[0], fp).wait_send()
    remote(wd, wp, wp_s, wp_r, sib).wait_send()
    remote(xs.at[1], xs.at[1], pu_s, pu_r.at[0, 0], sib).wait_send()
    sent = xs.at[0, :, pl.ds(0, 2 * (side * side - 1) * hr // side)]
    remote(sent, sent, ag_s, ag_r.at[0, 2], fp).wait_send()


def build(mesh, tn, dt):
    side = math.isqrt(mesh.shape["tp"] // 2)

    def step(x, w_gate, w_up, w_down):
        rows, d = x.shape
        hid = w_gate.shape[1]
        hr = rows // 2
        nt, nd = hid // tn, d // dt
        dma = pltpu.SemaphoreType.DMA
        hbm = pl.BlockSpec(memory_space=pltpu.HBM)
        m = side * rows
        result = pl.pallas_call(
            functools.partial(kernel, side, tn, dt),
            out_shape=(
                jax.ShapeDtypeStruct((rows, d), BF16),
                jax.ShapeDtypeStruct((2, side, m, d), BF16),
                jax.ShapeDtypeStruct((hid, d), BF16),
                jax.ShapeDtypeStruct((side - 1, nd, m, dt), BF16),
            ),
            in_specs=[hbm] * 4,
            out_specs=[hbm] * 4,
            scratch_shapes=[
                pltpu.VMEM((2, 2, d, tn), BF16),
                pltpu.VMEM((m, 2 * hid), BF16),
                pltpu.VMEM((2 * m, 2 * hid), BF16),
                pltpu.VMEM((nd, m, dt), BF16),
                pltpu.VMEM((2, m, dt), BF16),
                dma((2, 2)),
                dma((3,)),
                dma((2,)),
                dma,
                dma,
                dma((side, 2 * side)),
                dma,
                dma((side, 2 * side)),
                dma,
                dma,
                dma((6,)),
                dma((6,)),
                dma,
                dma,
                dma((nd,)),
                dma((side - 1, nd)),
                dma,
                dma((2 * nd,)),
                dma,
                dma((2 * nd,)),
                pltpu.SemaphoreType.REGULAR,
                pltpu.SemaphoreType.REGULAR,
            ],
            compiler_params=pltpu.CompilerParams(collective_id=0, has_side_effects=True, vmem_limit_bytes=67043328),
            cost_estimate=pl.CostEstimate(flops=6 * side * side * 2 * rows * d * hid, bytes_accessed=9 * d * hid * 4, transcendentals=0),
            name="mlp",
        )(x, w_gate, w_up, w_down)
        return result[0]

    return jax.shard_map(
        step,
        mesh=mesh,
        in_specs=(P(("dp", "tp"), None), P(None, "tp"), P(None, "tp"), P("tp", None)),
        out_specs=P(("dp", "tp"), None),
        check_vma=False,
    )


def solution(mesh):
    return build(mesh, 256, 1024)
```

```python
import functools
import math

import jax
import jax.numpy as jnp
from jax import lax
from jax.experimental import pallas as pl
from jax.experimental.pallas import tpu as pltpu
from jax.sharding import PartitionSpec as P

F32, BF16 = jnp.float32, jnp.bfloat16


def kernel(side, tn, dt, x, wg, wu, wd, y, xs, wp, rs, wbuf, h0, hk, out, inb, wsem, xsem, isem, ysem,
           ag_s, ag_r, pu_s, pu_r, wp_s, wp_r, hx_s, hx_r, hy_s, hy_r, rs_s, rs_r, a_s, a_r, b_s, b_r, hfree, nfree):
    rows, d = x.shape
    hid = wg.shape[1]
    hr = rows // 2
    half_rows = side * hr
    m = 2 * half_rows
    seg = 2 * hr
    nt, nd = hid // tn, d // dt
    sub = dt // tn
    cuts = (0, nt // 3, nt - 1, nt)
    parts = len(cuts) - 1
    pieces = 2 * nt
    dt2, ne = dt // 2, 2 * nd

    t = lax.axis_index("tp")
    c = lax.rem(t, 2)
    cx, cy = t // (2 * side), lax.rem(t // 2, side)
    f, s = cx * (1 - c) + cy * c, cy * (1 - c) + cx * c

    def at(df, ds):
        ff, ss = lax.rem(f + df + side, side), lax.rem(s + ds + side, side)
        return ((ff * (1 - c) + ss * c) * side + ss * (1 - c) + ff * c) * 2 + c

    fp, fm, sp, sm, sib = at(1, 0), at(-1, 0), at(0, 1), at(0, -1), t + 1 - 2 * c

    def remote(src, dst, send, recv, dev):
        return pltpu.make_async_remote_copy(src_ref=src, dst_ref=dst, send_sem=send, recv_sem=recv, device_id={"tp": dev})

    def when(cond):
        return pl.when(cond)

    def row0(j, hf):
        return hf * half_rows + j * hr

    def piece(k, j, hf, other=0):
        return xs.at[other, k, pl.ds(row0(j, hf), hr)]

    def source(k, j, hf):
        if isinstance(k, int) and isinstance(j, int) and k == 0 and j == 0:
            return x.at[pl.ds(hf * hr, hr)]
        return piece(k, j, hf)

    def move(src, k, j, hf, dev):
        i = j * 2 + hf
        return remote(src, piece(k, j, hf), ag_s, ag_r.at[k, i], dev)

    def hand(k, j, hf):
        i = j * 2 + hf
        return remote(source(k, j, hf), piece(k, j, hf, 1), pu_s, pu_r.at[k, i], sib)

    def arrive(k, j, hf):
        move(piece(k, j, hf), k, j, hf, sib).wait_recv()
        hand(k, j, hf).start()

    def push(k, j):
        for hf in range(2):
            arrive(k, j, hf)

    def forward(k, j):
        for hf, dev in ((0, sp), (1, sm)):
            move(source(k, j, hf), k + 1, j, hf, dev).start()

    def far(k, hf):
        move(piece(k, 1 + hf, hf), k, 3, hf, (fp, fm)[hf]).start()

    def load(xb, slot, row, src, size, sem):
        pltpu.make_async_copy(src, xb.at[slot, pl.ds(row, size)], xsem.at[sem]).start()

    def loaded(xb, slot, row, size, sem):
        dst = xb.at[slot, pl.ds(row, size)]
        pltpu.make_async_copy(dst, dst, xsem.at[sem]).wait()

    def load_small(xb, i, k, j, hf):
        if i < 2:
            src = source(k, j, hf)
        else:
            hand(k, j, hf).wait_recv()
            src = piece(k, j, hf, 1)
        load(xb, 0, i * hr, src, hr, 0)

    def load_mid(xb, other, hf):
        if other:
            for j in (1, 2):
                hand(0, j, hf).wait_recv()
        load(xb, 1, (2 * hf + other) * seg, xs.at[other, 0, pl.ds(row0(1, hf), seg)], seg, 1 + hf)

    def load_pair(xb, slot, i, other, k, pair, hf):
        for q in range(2):
            @when(other == 1)
            def _():
                hand(k, 2 * pair + q, hf).wait_recv()
        load(xb, slot, i * seg, xs.at[other, k, pl.ds(hf * half_rows + pair * seg, seg)], seg, slot)

    def load_one(xb, slot, i, k, j, hf):
        hand(k, j, hf).wait_recv()
        load(xb, slot, i * seg + (j % 2) * hr, piece(k, j, hf, 1), hr, slot)

    def u_part(n, z, slot):
        cols, depth = pl.ds(pl.multiple_of(n * tn, tn), tn), pl.ds(z * (d // 2), d // 2)
        return [pltpu.make_async_copy(w.at[depth, cols], wbuf.at[slot, i, depth], wsem.at[slot, z]) for i, w in enumerate((wg, wu))]

    def u_copies(n, slot):
        return u_part(n, 0, slot) + u_part(n, 1, slot)

    def d_rows(q):
        return q // 2, (q % 2) * 2 * hid

    def d_copies(n, slot):
        r = []
        for q in range(sub):
            p, o = d_rows(q)
            cols = pl.ds(pl.multiple_of(n * dt + q * tn, tn), tn)
            for i, w in enumerate((wd, wp)):
                r.append(pltpu.make_async_copy(w.at[:, cols], wbuf.at[slot, p, pl.ds(o + i * hid, hid)], wsem.at[slot, 0]))
        return r

    def start(copies):
        for cp in copies:
            cp.start()

    def held(slot, z, depth):
        dst = wbuf.at[slot, :, depth]
        pltpu.make_async_copy(dst, dst, wsem.at[slot, z]).wait()

    def u_held(z, slot):
        held(slot, z, pl.ds(z * (d // 2), d // 2))

    def d_held(slot):
        held(slot, 0, pl.ds(0, sub * hid))

    def cut(part):
        return cuts[part] * tn, (cuts[part + 1] - cuts[part]) * tn

    def h_copy(hdst, idx, part, src, dst, size):
        lo, width = cut(part)
        return remote(hk.at[pl.ds(m + src, size), pl.ds(lo, width)], hdst.at[pl.ds(dst, size), pl.ds(hid + lo, width)],
                      hx_s.at[idx], hx_r.at[idx], sib)

    def h_push(hdst, idx, part, src, dst, size):
        for q in range(2):
            h_copy(hdst, idx, part, src[q], dst[q], size).start()

    def h_all(idx, size):
        r = pl.ds(0, 2 * size)
        return remote(hk.at[r, pl.ds(0, hid)], hk.at[r, pl.ds(hid, hid)], hx_s.at[idx], hx_r.at[idx], sib)

    def h_sent(idx, size):
        h_all(idx, size).wait_send()

    def h_here(idx, size):
        h_all(idx, size).wait_recv()

    def hy_copy(lo, size):
        return remote(hk.at[pl.ds(m, m), pl.ds(lo, size)], hk.at[pl.ds(0, m), pl.ds(hid + lo, size)], hy_s, hy_r, sib)

    def hy_all():
        return hy_copy(0, hid)

    def w_piece(i):
        r = pl.ds(i * (hid // pieces), hid // pieces)
        return remote(wd.at[r], wp.at[r], wp_s, wp_r, sib)

    def w_pieces(lo, hi):
        for i in range(lo, hi):
            w_piece(i).start()

    def hidden(lhs, ws):
        gate = jnp.dot(lhs[...], wbuf[ws, 0], preferred_element_type=F32)
        up = jnp.dot(lhs[...], wbuf[ws, 1], preferred_element_type=F32)
        return (jax.nn.silu(gate) * up).astype(BF16)

    def u_cols(i):
        return pl.ds(pl.multiple_of(i * tn, tn), tn)

    def u_small(xb, slot, row, sem, keep, where, idx, hook, end, ahead, nxt):
        half = d // 2

        def after(i, more):
            return lax.rem(i + more, end) if nxt == 2 else i + more

        def body(i, carry):
            ws = lax.rem(i, 2)
            hook(i)

            for part in range(parts):
                if cuts[part + 1] < end:
                    @when(i == cuts[part + 1])
                    def _():
                        h_push(h0, idx, part, keep, where, hr)

            if not ahead:
                @when(i == 0)
                def _():
                    start(u_part(1, 0, 1))

            if nxt:
                start(u_part(after(i, 1), 1, 1 - ws))
            else:
                @when(i < end - 1)
                def _():
                    start(u_part(i + 1, 1, 1 - ws))

                @when(i == end - 1)
                def _():
                    start(d_copies(0, 0))

            @when(i == 0)
            def _():
                loaded(xb, slot, row, 4 * hr, sem)

            def products_of(z):
                u_held(z, ws)
                depth = pl.ds(z * half, half)
                lhs = xb[slot, pl.ds(row, 4 * hr), depth]
                return [jnp.dot(lhs, wbuf[ws, q, depth], preferred_element_type=F32) for q in range(2)]

            gate, up = products_of(0)

            if nxt == 2:
                start(u_part(after(i, 2), 0, ws))
            else:
                @when(i < end - 2 + nxt)
                def _():
                    start(u_part(i + 2, 0, ws))

            gate2, up2 = products_of(1)
            h = (jax.nn.silu(gate + gate2) * (up + up2)).astype(BF16)
            for q in range(2):
                h0[pl.ds(where[q], hr), u_cols(i)] = h[q * hr : (q + 1) * hr]
                hk[pl.ds(m + keep[q], hr), u_cols(i)] = h[(2 + q) * hr : (3 + q) * hr]
            return carry

        lax.fori_loop(0, end, body, 0)
        for part in range(parts):
            if cuts[part + 1] == end:
                h_push(h0, idx, part, keep, where, hr)

    def u_big(xb, keep, where, idx, hook, begin):
        def body(i, carry):
            ws = lax.rem(i, 2)
            hook(i)

            for part in range(1, parts - 1):
                @when(i == cuts[part + 1])
                def _():
                    h_push(h0, idx, part, keep, where, seg)

            start(u_copies(lax.rem(i + 1, nt), 1 - ws))
            u_held(0, ws)
            u_held(1, ws)
            h = hidden(xb.at[1], ws)
            for q in range(2):
                h0[pl.ds(where[q], seg), u_cols(i)] = h[2 * q * seg : (2 * q + 1) * seg]
                hk[pl.ds(m + keep[q], seg), u_cols(i)] = h[(2 * q + 1) * seg : (2 * q + 2) * seg]
            return carry

        lax.fori_loop(begin, nt, body, 0)
        h_push(h0, idx, parts - 1, keep, where, seg)

    def sum_copy(hop, n, hf):
        part = pl.ds(hf * half_rows, half_rows)
        return remote(out.at[n, part], rs.at[hop, n, part], rs_s.at[n], rs_r.at[hop, n], (sp, sm)[hf])

    def sum_all(hop, n):
        return remote(out.at[n], rs.at[hop, n], rs_s.at[n], rs_r.at[hop, n], sp)

    def in_copy(hop, n):
        b = lax.rem(n, 2)
        return pltpu.make_async_copy(rs.at[hop, n], inb.at[b], isem.at[b])

    def in_start(hop, n):
        sum_all(hop, n).wait_recv()
        in_copy(hop, n).start()

    def products(h, n, q):
        p, o = d_rows(q)
        ws = lax.rem(n, 2)
        cols = slice(q * tn, (q + 1) * tn)
        term = jnp.dot(h[...], wbuf[ws, p, pl.ds(o, 2 * hid)], preferred_element_type=F32)
        return term + inb[lax.rem(n, 2), :, cols].astype(F32), cols

    def step_cols(e, base=0):
        return pl.ds(pl.multiple_of(base + lax.rem(e, 2) * dt2, dt2), dt2)

    def land(e, i):
        r = pl.ds(pl.multiple_of((e // 2) * rows, rows), rows)
        return hk.at[r, step_cols(e, i * dt)]

    def leave(e, row, size):
        return out.at[e // 2, pl.ds(row, size), step_cols(e)]

    def a_copy(e, hf):
        return remote(leave(e, hf * hr, hr), land(e, 2).at[pl.ds(hf * hr, hr)], a_s, a_r.at[e], (fp, fm)[hf])

    def b_copy(e, i):
        return remote(leave(e, (1 + i) * rows, rows), land(e, i), b_s, b_r.at[e], (fp, fm)[i])

    def y_copy(e):
        cols = pl.ds(pl.multiple_of(e * dt2, dt2), dt2)
        return pltpu.make_async_copy(leave(e, 3 * rows, rows), y.at[:, cols], ysem)

    def rounds(xb):
        start(u_copies(0, 0))
        start(u_part(1, 0, 1))
        for i in range(2):
            load_small(xb, i, 0, 0, i)
        barrier = pltpu.get_barrier_semaphore()
        for dev in (fp, fm, sp, sm, sib):
            pl.semaphore_signal(barrier, 1, device_id={"tp": dev})
        pl.semaphore_wait(barrier, 5)

        for hf in range(2):
            hand(0, 0, hf).start()
        for hf in range(2):
            move(source(0, 0, hf), 0, 1, hf, fp).start()
            move(source(0, 0, hf), 0, 2, hf, fm).start()
        inb[...] = jnp.zeros_like(inb)
        for i in range(2, 4):
            load_small(xb, i, 0, 0, i - 2)

        def on(i, v, *calls):
            @when(i == v)
            def _():
                for fn, *a in calls:
                    fn(*a)

        def hook(i):
            on(i, nt - 3, (arrive, 0, 1, 0), (arrive, 0, 2, 0), (load_mid, xb, 0, 0))
            on(i, nt - 1, (load_mid, xb, 1, 0))

        u_small(xb, 0, 0, 0, (0, hr), (row0(0, 0), row0(0, 1)), 0, hook, nt, True, 2)

        def hook(i):
            on(i, 0, (forward, 0, 0))
            on(i, 1, (arrive, 0, 1, 1), (arrive, 0, 2, 1), (forward, 0, 1), (load_mid, xb, 0, 1))

        u_small(xb, 1, 0, 1, (seg, seg + hr), (row0(1, 0), row0(2, 0)), 1, hook, cuts[1], True, 2)
        load_mid(xb, 1, 1)

        def hook(i):
            on(i, 1, (w_pieces, 0, 1))

        u_small(xb, 1, 2 * seg, 2, (half_rows + seg, half_rows + seg + hr), (row0(1, 1), row0(2, 1)), 1, hook, cuts[1], True, 1)

        def hook(i):
            on(i, cuts[1], (w_pieces, 1, 3))
            on(i, nt - 3, (w_pieces, 3, 4))
            on(i, nt - 2, (forward, 0, 2), (push, 1, 0))
            on(i, nt - 1, (push, 1, 1), (load_pair, xb, 0, 0, 0, 1, 0, 0), (load_pair, xb, 0, 1, 0, 1, 0, 1),
               (load_one, xb, 0, 2, 1, 0, 0), (load_one, xb, 0, 3, 1, 0, 1))

        u_big(xb, (seg, half_rows + seg), (row0(1, 0), row0(1, 1)), 1, hook, cuts[1])
        for hf in range(2):
            load_one(xb, 0, 2 + hf, 1, 1, hf)

        def one_round(k, carry):
            fi = 2 // (k + 1)
            first = k == 1

            def up(it, carry):
                b = fi * (it // nt) + (1 - fi) * lax.rem(it, 2)
                i = fi * lax.rem(it, nt) + (1 - fi) * (it // 2)
                ws = lax.rem(i, 2)

                @when(first)
                def _():
                    def keep(c):
                        return (c * seg, half_rows + c * seg)

                    def where(c):
                        return (row0(2 * c, 0), row0(2 * c, 1))

                    def h_parts(c):
                        for part in range(parts - 1):
                            on(it, c * nt + cuts[part + 1], (h_push, hk, 3 + c, part, keep(c), where(c), seg))

                    @when(it < nt)
                    def _():
                        on(it, 0, (h_sent, 0, hr), (far, 1, 0), (w_pieces, 4, 5))
                        on(it, 1, (push, 1, 2), (far, 1, 1))
                        on(it, 4, (push, 1, 3), (forward, 1, 0), (load_pair, xb, 1, 0, 0, 1, 1, 0), (load_pair, xb, 1, 1, 0, 1, 1, 1),
                           (w_pieces, 5, 6))
                        on(it, 5, (w_pieces, 6, 8), (load_pair, xb, 1, 2, 1, 1, 1, 0), (load_pair, xb, 1, 3, 1, 1, 1, 1))
                        h_parts(0)

                    @when(it >= nt)
                    def _():
                        @when(it < pieces - 2)
                        def _():
                            w_piece(it + 2).start()

                        on(it, nt, (h_push, hk, 3, parts - 1, keep(0), where(0), seg), (h_sent, 1, seg), (forward, 1, 1))
                        on(it, 7, (forward, 1, 2))
                        on(it, 8, (forward, 1, 3))
                        on(it, 9, (push, 2, 0))
                        on(it, 11, (push, 2, 1))
                        h_parts(1)

                @when(k > 1)
                def _():
                    on(it, 2 * nt - 2, (in_start, k - 2, 0))
                    for part in range(1, parts):
                        @when(it == 2 * nt - 3 + part)
                        def _():
                            hy_copy(*cut(part)).start()

                @when(first & (it < 2 * nt - 1))
                def _():
                    start(u_copies(lax.rem(i + 1, nt), 1 - ws))

                @when(it == 2 * nt - 1)
                def _():
                    @when(first)
                    def _():
                        remote(wd, wp, wp_s, wp_r, sib).wait_recv()

                    start(d_copies(0, 0))

                @when(first & (i == 0))
                def _():
                    loaded(xb, b, 0, 4 * seg, b)

                @when(first | (b == 0))
                def _():
                    u_held(0, ws)
                    u_held(1, ws)

                h = hidden(xb.at[b], ws)
                for q in range(4):
                    r = fi * (q * half_rows + b * seg) + (1 - fi) * ((1 - b) * m + q * seg)
                    hk[pl.ds(pl.multiple_of(r, seg), seg), u_cols(i)] = h[q * seg : (q + 1) * seg]
                return carry

            def up_both(i, carry):
                ws = lax.rem(i, 2)
                start(u_copies(i + 1, 1 - ws))

                @when(k == 2)
                def _():
                    on(i, 0, (h_sent, 3, seg), (h_sent, 4, seg))
                    on(i, 2, (push, 3, 0))
                    on(i, 4, (push, 3, 1))

                @when(k == 3)
                def _():
                    on(i, 4, (push, 0, 3))

                    @when(i == 0)
                    def _():
                        hy_all().wait_send()

                @when(i == cuts[1])
                def _():
                    pl.semaphore_wait(hfree, 1)
                    hy_copy(*cut(0)).start()

                @when(i == 0)
                def _():
                    for slot in range(2):
                        loaded(xb, slot, 0, 4 * seg, slot)

                u_held(0, ws)
                u_held(1, ws)
                hk[pl.ds(m, m), u_cols(i)] = hidden(xb.at[0], ws)
                hk[pl.ds(0, m), u_cols(i)] = hidden(xb.at[1], ws)
                return carry

            lax.fori_loop(0, (1 - fi) * (nt - 1), up_both, 0)
            lax.fori_loop((1 - fi) * 2 * (nt - 1), 2 * nt, up, 0)

            @when(first)
            def _():
                h_push(hk, 4, parts - 1, (seg, half_rows + seg), (row0(2, 0), row0(2, 1)), seg)
                h_here(3, seg)
                h_here(4, seg)

            @when(k > 1)
            def _():
                hy_all().wait_recv()

            def down(n, carry):
                ws = lax.rem(n, 2)

                @when(n < nd - 1)
                def _():
                    start(d_copies(n + 1, 1 - ws))

                @when(n == nd - 1)
                def _():
                    start(u_copies(0, 0))

                @when(k > 1)
                def _():
                    in_copy(k - 2, n).wait()

                    @when(n < nd - 1)
                    def _():
                        in_start(k - 2, n + 1)

                    sum_all(0, n).wait_send()

                @when(first)
                def _():
                    on(n, 1, (push, 2, 2))
                    on(n, 4, (push, 2, 3))

                    @when(lax.rem(n, 2) == 0)
                    def _():
                        forward(2, n // 2)

                @when(k == 2)
                def _():
                    on(n, 2, (push, 3, 2))
                    on(n, 4, (push, 3, 3))
                    on(n, 7, (far, 0, 0), (far, 0, 1))

                @when((k < 3) & ((n == 1) | (n == 3) | (n == 5) | (n == 6)))
                def _():
                    other, pair = lax.rem(n // 2, 2), n // (nd // 2)
                    for hf in range(2):
                        load_pair(xb, 1 - other, 2 * hf + pair, other, k + 1, pair, hf)

                @when(k == 3)
                def _():
                    for q in range(4):
                        on(n, 2 + q, (load_small, xb, q, 0, 3, q % 2))

                d_held(ws)
                for q in range(sub):
                    total, cols = products(hk.at[pl.ds(0, m)], n, q)
                    out[n, :, cols] = total.astype(BF16)
                for hf in range(2):
                    sum_copy(k - 1, n, hf).start()
                return carry

            lax.fori_loop(0, nd, down, 0)

            @when(k < 3)
            def _():
                pl.semaphore_signal(hfree, 1, device_id={"tp": sib})

            return carry

        lax.fori_loop(1, side, one_round, 0)

        def hook(i):
            on(i, nt - 2, (in_start, 2, 0))

        hy_all().wait_send()
        u_small(xb, 0, 0, 0, (0, hr), (row0(3, 0), row0(3, 1)), 5, hook, nt, False, 0)

    pl.run_scoped(rounds, pltpu.VMEM((2, 8 * hr, d), BF16))

    def last(t0, t1, t2):
        h_sent(5, hr)
        for dev in (fp, fm):
            pl.semaphore_signal(nfree, 1, device_id={"tp": dev})
        for idx, size in ((0, hr), (1, seg), (5, hr)):
            h_here(idx, size)

        def add_far(e):
            both = pl.ds(0, rows)
            remote(out.at[0, both, pl.ds(0, dt2)], land(e, 2), a_s, a_r.at[e], fp).wait_recv()
            far_in = land(e, 2)[...].astype(F32)
            leave(e, rows, hr)[...] = (t2[e, :hr] + far_in[:hr]).astype(BF16)
            leave(e, rows + hr, hr)[...] = t2[e, hr:].astype(BF16)
            leave(e, 2 * rows, hr)[...] = t1[e, :hr].astype(BF16)
            leave(e, 2 * rows + hr, hr)[...] = (t1[e, hr:] + far_in[hr:]).astype(BF16)
            for i in range(2):
                b_copy(e, i).start()

        def add_near(e):
            both = pl.ds(0, 2 * rows)
            remote(out.at[0, both, pl.ds(0, dt2)], out.at[0, both, pl.ds(0, dt2)], b_s, b_r.at[e], fp).wait_recv()
            leave(e, 3 * rows, rows)[...] = (t0[e] + land(e, 0)[...].astype(F32) + land(e, 1)[...].astype(F32)).astype(BF16)
            y_copy(e).start()

        def down(e, carry):
            n, c2 = e // 2, lax.rem(e, 2)
            ws = lax.rem(n, 2)

            @when(c2 == 0)
            def _():
                @when(n < nd - 1)
                def _():
                    start(d_copies(n + 1, 1 - ws))

                in_copy(2, n).wait()

                @when(n < nd - 1)
                def _():
                    in_start(2, n + 1)

                sum_all(0, n).wait_send()
                d_held(ws)

            @when(e >= 3)
            def _():
                add_far(e - 3)

            @when(e >= 6)
            def _():
                add_near(e - 6)

            for q in range(2):
                term = jnp.dot(h0[...], wbuf[ws, c2, pl.ds(q * 2 * hid, 2 * hid)], preferred_element_type=F32)
                cols = slice(q * tn, (q + 1) * tn)
                total = term + inb[lax.rem(n, 2), :, pl.ds(pl.multiple_of(c2 * dt2 + q * tn, tn), tn)].astype(F32)
                for hf in range(2):
                    o = hf * half_rows
                    dst = pl.ds(hf * hr, hr)
                    t0[e, dst, cols] = total[o : o + hr]
                    t1[e, dst, cols] = total[o + hr : o + 2 * hr]
                    t2[e, dst, cols] = total[o + 2 * hr : o + 3 * hr]
                    out[n, dst, pl.ds(pl.multiple_of(c2 * dt2 + q * tn, tn), tn)] = total[o + 3 * hr : o + 4 * hr].astype(BF16)

            @when(e == 0)
            def _():
                pl.semaphore_wait(nfree, 2)

            for hf in range(2):
                a_copy(e, hf).start()
            return carry

        lax.fori_loop(0, ne, down, 0)
        for i in range(3):
            add_near(ne - 6 + i)
            add_far(ne - 3 + i)
        for i in range(3):
            add_near(ne - 3 + i)

    shape = pltpu.VMEM((ne, rows, dt2), F32)
    pl.run_scoped(last, shape, shape, shape)

    pltpu.make_async_copy(y, y, ysem).wait()
    for sem, r in ((a_s, pl.ds(0, rows)), (b_s, pl.ds(rows, 2 * rows))):
        remote(out.at[:, r], out.at[:, r], sem, a_r.at[0], fp).wait_send()
    remote(wd, wp, wp_s, wp_r, sib).wait_send()
    remote(xs.at[1], xs.at[1], pu_s, pu_r.at[0, 0], sib).wait_send()
    sent = xs.at[0, :, pl.ds(0, 2 * (side * side - 1) * hr // side)]
    remote(sent, sent, ag_s, ag_r.at[0, 2], fp).wait_send()


def build(mesh, tn, dt):
    side = math.isqrt(mesh.shape["tp"] // 2)

    def step(x, w_gate, w_up, w_down):
        rows, d = x.shape
        hid = w_gate.shape[1]
        hr = rows // 2
        nt, nd = hid // tn, d // dt
        dma = pltpu.SemaphoreType.DMA
        hbm = pl.BlockSpec(memory_space=pltpu.HBM)
        m = side * rows
        result = pl.pallas_call(
            functools.partial(kernel, side, tn, dt),
            out_shape=(
                jax.ShapeDtypeStruct((rows, d), BF16),
                jax.ShapeDtypeStruct((2, side, m, d), BF16),
                jax.ShapeDtypeStruct((hid, d), BF16),
                jax.ShapeDtypeStruct((side - 1, nd, m, dt), BF16),
            ),
            in_specs=[hbm] * 4,
            out_specs=[hbm] * 4,
            scratch_shapes=[
                pltpu.VMEM((2, 2, d, tn), BF16),
                pltpu.VMEM((m, 2 * hid), BF16),
                pltpu.VMEM((2 * m, 2 * hid), BF16),
                pltpu.VMEM((nd, m, dt), BF16),
                pltpu.VMEM((2, m, dt), BF16),
                dma((2, 2)),
                dma((3,)),
                dma((2,)),
                dma,
                dma,
                dma((side, 2 * side)),
                dma,
                dma((side, 2 * side)),
                dma,
                dma,
                dma((6,)),
                dma((6,)),
                dma,
                dma,
                dma((nd,)),
                dma((side - 1, nd)),
                dma,
                dma((2 * nd,)),
                dma,
                dma((2 * nd,)),
                pltpu.SemaphoreType.REGULAR,
                pltpu.SemaphoreType.REGULAR,
            ],
            compiler_params=pltpu.CompilerParams(collective_id=0, has_side_effects=True, vmem_limit_bytes=67043328),
            cost_estimate=pl.CostEstimate(flops=6 * side * side * 2 * rows * d * hid, bytes_accessed=9 * d * hid * 4, transcendentals=0),
            name="mlp",
        )(x, w_gate, w_up, w_down)
        return result[0]

    return jax.shard_map(
        step,
        mesh=mesh,
        in_specs=(P(("dp", "tp"), None), P(None, "tp"), P(None, "tp"), P("tp", None)),
        out_specs=P(("dp", "tp"), None),
        check_vma=False,
    )


def solution(mesh):
    return build(mesh, 256, 1024)
```

```python
import functools
import math

import jax
import jax.numpy as jnp
from jax import lax
from jax.experimental import pallas as pl
from jax.experimental.pallas import tpu as pltpu
from jax.sharding import PartitionSpec as P

F32, BF16 = jnp.float32, jnp.bfloat16


def kernel(side, tn, dt, x, wg, wu, wd, y, xs, wp, rs, wbuf, h0, hk, out, inb, wsem, xsem, isem, ysem,
           ag_s, ag_r, pu_s, pu_r, wp_s, wp_r, hx_s, hx_r, hy_s, hy_r, rs_s, rs_r, a_s, a_r, b_s, b_r, hfree, nfree):
    rows, d = x.shape
    hid = wg.shape[1]
    hr = rows // 2
    half_rows = side * hr
    m = 2 * half_rows
    seg = 2 * hr
    nt, nd = hid // tn, d // dt
    sub = dt // tn
    cuts = (0, nt // 3, nt - 1, nt)
    parts = len(cuts) - 1
    pieces = 2 * nt
    dt2, ne = dt // 2, 2 * nd

    t = lax.axis_index("tp")
    c = lax.rem(t, 2)
    cx, cy = t // (2 * side), lax.rem(t // 2, side)
    f, s = cx * (1 - c) + cy * c, cy * (1 - c) + cx * c

    def at(df, ds):
        ff, ss = lax.rem(f + df + side, side), lax.rem(s + ds + side, side)
        return ((ff * (1 - c) + ss * c) * side + ss * (1 - c) + ff * c) * 2 + c

    fp, fm, sp, sm, sib = at(1, 0), at(-1, 0), at(0, 1), at(0, -1), t + 1 - 2 * c

    def remote(src, dst, send, recv, dev):
        return pltpu.make_async_remote_copy(src_ref=src, dst_ref=dst, send_sem=send, recv_sem=recv, device_id={"tp": dev})

    def when(cond):
        return pl.when(cond)

    def row0(j, hf):
        return hf * half_rows + j * hr

    def piece(k, j, hf, other=0):
        return xs.at[other, k, pl.ds(row0(j, hf), hr)]

    def source(k, j, hf):
        if isinstance(k, int) and isinstance(j, int) and k == 0 and j == 0:
            return x.at[pl.ds(hf * hr, hr)]
        return piece(k, j, hf)

    def move(src, k, j, hf, dev):
        i = j * 2 + hf
        return remote(src, piece(k, j, hf), ag_s, ag_r.at[k, i], dev)

    def hand(k, j, hf):
        i = j * 2 + hf
        return remote(source(k, j, hf), piece(k, j, hf, 1), pu_s, pu_r.at[k, i], sib)

    def arrive(k, j, hf):
        move(piece(k, j, hf), k, j, hf, sib).wait_recv()
        hand(k, j, hf).start()

    def landed(k, j):
        for hf in range(2):
            move(piece(k, j, hf), k, j, hf, sib).wait_recv()

    def give(k, j):
        for hf in range(2):
            hand(k, j, hf).start()

    def push(k, j):
        for hf in range(2):
            arrive(k, j, hf)

    def forward(k, j):
        for hf, dev in ((0, sp), (1, sm)):
            move(source(k, j, hf), k + 1, j, hf, dev).start()

    def far(k, hf):
        move(piece(k, 1 + hf, hf), k, 3, hf, (fp, fm)[hf]).start()

    def load(xb, slot, row, src, size, sem):
        pltpu.make_async_copy(src, xb.at[slot, pl.ds(row, size)], xsem.at[sem]).start()

    def loaded(xb, slot, row, size, sem):
        dst = xb.at[slot, pl.ds(row, size)]
        pltpu.make_async_copy(dst, dst, xsem.at[sem]).wait()

    def load_small(xb, i, k, j, hf):
        if i < 2:
            src = source(k, j, hf)
        else:
            hand(k, j, hf).wait_recv()
            src = piece(k, j, hf, 1)
        load(xb, 0, i * hr, src, hr, 0)

    def load_mid(xb, other, hf):
        if other:
            for j in (1, 2):
                hand(0, j, hf).wait_recv()
        load(xb, 1, (2 * hf + other) * seg, xs.at[other, 0, pl.ds(row0(1, hf), seg)], seg, 1 + hf)

    def load_pair(xb, slot, i, other, k, pair, hf):
        for q in range(2):
            @when(other == 1)
            def _():
                hand(k, 2 * pair + q, hf).wait_recv()
        load(xb, slot, i * seg, xs.at[other, k, pl.ds(hf * half_rows + pair * seg, seg)], seg, slot)

    def load_one(xb, slot, i, k, j, hf):
        hand(k, j, hf).wait_recv()
        load(xb, slot, i * seg + (j % 2) * hr, piece(k, j, hf, 1), hr, slot)

    def u_part(n, z, slot):
        cols, depth = pl.ds(pl.multiple_of(n * tn, tn), tn), pl.ds(z * (d // 2), d // 2)
        return [pltpu.make_async_copy(w.at[depth, cols], wbuf.at[slot, depth, pl.ds(i * tn, tn)], wsem.at[slot, z])
                for i, w in enumerate((wg, wu))]

    def u_copies(n, slot):
        return u_part(n, 0, slot) + u_part(n, 1, slot)

    def d_copies(n, slot):
        r = []
        for p in range(2):
            cols = pl.ds(pl.multiple_of(n * dt + p * dt2, dt2), dt2)
            for i, w in enumerate((wd, wp)):
                rows_p = pl.ds((2 * p + i) * hid, hid)
                r.append(pltpu.make_async_copy(w.at[:, cols], wbuf.at[slot, rows_p], wsem.at[slot, 0]))
        return r

    def start(copies):
        for cp in copies:
            cp.start()

    def held(slot, z, depth):
        dst = wbuf.at[slot, depth]
        pltpu.make_async_copy(dst, dst, wsem.at[slot, z]).wait()

    def u_held(z, slot):
        held(slot, z, pl.ds(z * (d // 2), d // 2))

    def d_held(slot):
        held(slot, 0, pl.ds(0, 4 * hid))

    def cut(part):
        return cuts[part] * tn, (cuts[part + 1] - cuts[part]) * tn

    def h_copy(hdst, idx, part, src, dst, size):
        lo, width = cut(part)
        return remote(hk.at[pl.ds(m + src, size), pl.ds(lo, width)], hdst.at[pl.ds(dst, size), pl.ds(hid + lo, width)],
                      hx_s.at[idx], hx_r.at[idx], sib)

    def h_push(hdst, idx, part, src, dst, size):
        for q in range(2):
            h_copy(hdst, idx, part, src[q], dst[q], size).start()

    def h_all(idx, size):
        r = pl.ds(0, 2 * size)
        return remote(hk.at[r, pl.ds(0, hid)], hk.at[r, pl.ds(hid, hid)], hx_s.at[idx], hx_r.at[idx], sib)

    def h_sent(idx, size):
        h_all(idx, size).wait_send()

    def h_here(idx, size):
        h_all(idx, size).wait_recv()

    def hy_copy(lo, size):
        return remote(hk.at[pl.ds(m, m), pl.ds(lo, size)], hk.at[pl.ds(0, m), pl.ds(hid + lo, size)], hy_s, hy_r, sib)

    def hy_all():
        return hy_copy(0, hid)

    def w_piece(i):
        r = pl.ds(i * (hid // pieces), hid // pieces)
        return remote(wd.at[r], wp.at[r], wp_s, wp_r, sib)

    def w_pieces(lo, hi):
        for i in range(lo, hi):
            w_piece(i).start()

    def hidden(lhs, ws):
        gate = jnp.dot(lhs[...], wbuf[ws, :, :tn], preferred_element_type=F32)
        up = jnp.dot(lhs[...], wbuf[ws, :, tn:], preferred_element_type=F32)
        return (jax.nn.silu(gate) * up).astype(BF16)

    def u_cols(i):
        return pl.ds(pl.multiple_of(i * tn, tn), tn)

    def u_small(xb, slot, row, sem, keep, where, idx, hook, end, ahead, nxt):
        half = d // 2

        def after(i, more):
            return lax.rem(i + more, end) if nxt == 2 else i + more

        def body(i, carry):
            ws = lax.rem(i, 2)
            hook(i)

            for part in range(parts):
                if cuts[part + 1] < end:
                    @when(i == cuts[part + 1])
                    def _():
                        h_push(h0, idx, part, keep, where, hr)

            if not ahead:
                @when(i == 0)
                def _():
                    start(u_part(1, 0, 1))

            if nxt:
                start(u_part(after(i, 1), 1, 1 - ws))
            else:
                @when(i < end - 1)
                def _():
                    start(u_part(i + 1, 1, 1 - ws))

                @when(i == end - 1)
                def _():
                    start(d_copies(0, 0))

            @when(i == 0)
            def _():
                loaded(xb, slot, row, 4 * hr, sem)

            def products_of(z):
                u_held(z, ws)
                depth = pl.ds(z * half, half)
                lhs = xb[slot, pl.ds(row, 4 * hr), depth]
                return [jnp.dot(lhs, wbuf[ws, depth, q * tn : (q + 1) * tn], preferred_element_type=F32) for q in range(2)]

            gate, up = products_of(0)

            if nxt == 2:
                start(u_part(after(i, 2), 0, ws))
            else:
                @when(i < end - 2 + nxt)
                def _():
                    start(u_part(i + 2, 0, ws))

            gate2, up2 = products_of(1)
            h = (jax.nn.silu(gate + gate2) * (up + up2)).astype(BF16)
            for q in range(2):
                h0[pl.ds(where[q], hr), u_cols(i)] = h[q * hr : (q + 1) * hr]
                hk[pl.ds(m + keep[q], hr), u_cols(i)] = h[(2 + q) * hr : (3 + q) * hr]
            return carry

        lax.fori_loop(0, end, body, 0)
        for part in range(parts):
            if cuts[part + 1] == end:
                h_push(h0, idx, part, keep, where, hr)

    def u_big(xb, keep, where, idx, hook, begin):
        def body(i, carry):
            ws = lax.rem(i, 2)
            hook(i)

            for part in range(1, parts - 1):
                @when(i == cuts[part + 1])
                def _():
                    h_push(h0, idx, part, keep, where, seg)

            start(u_copies(lax.rem(i + 1, nt), 1 - ws))
            u_held(0, ws)
            u_held(1, ws)
            h = hidden(xb.at[1], ws)
            for q in range(2):
                h0[pl.ds(where[q], seg), u_cols(i)] = h[2 * q * seg : (2 * q + 1) * seg]
                hk[pl.ds(m + keep[q], seg), u_cols(i)] = h[(2 * q + 1) * seg : (2 * q + 2) * seg]
            return carry

        lax.fori_loop(begin, nt, body, 0)
        h_push(h0, idx, parts - 1, keep, where, seg)

    def sum_copy(hop, n, hf):
        part = pl.ds(hf * half_rows, half_rows)
        return remote(out.at[n, part], rs.at[hop, n, part], rs_s.at[n], rs_r.at[hop, n], (sp, sm)[hf])

    def sum_all(hop, n):
        return remote(out.at[n], rs.at[hop, n], rs_s.at[n], rs_r.at[hop, n], sp)

    def in_copy(hop, n):
        b = lax.rem(n, 2)
        return pltpu.make_async_copy(rs.at[hop, n], inb.at[b], isem.at[b])

    def in_start(hop, n):
        sum_all(hop, n).wait_recv()
        in_copy(hop, n).start()

    def products(h, n, q):
        ws = lax.rem(n, 2)
        cols = slice(q * tn, (q + 1) * tn)
        term = jnp.dot(h[...], wbuf[ws, pl.ds((q // 2) * 2 * hid, 2 * hid), (q % 2) * tn : (q % 2 + 1) * tn], preferred_element_type=F32)
        return term + inb[lax.rem(n, 2), :, cols].astype(F32), cols

    def step_cols(e, base=0):
        return pl.ds(pl.multiple_of(base + lax.rem(e, 2) * dt2, dt2), dt2)

    def land(e, i):
        r = pl.ds(pl.multiple_of((e // 2) * rows, rows), rows)
        return hk.at[r, step_cols(e, i * dt)]

    def leave(e, row, size):
        return out.at[e // 2, pl.ds(row, size), step_cols(e)]

    def a_copy(e, hf):
        return remote(leave(e, hf * hr, hr), land(e, 2).at[pl.ds(hf * hr, hr)], a_s, a_r.at[e], (fp, fm)[hf])

    def b_copy(e, i):
        return remote(leave(e, (1 + i) * rows, rows), land(e, i), b_s, b_r.at[e], (fp, fm)[i])

    def y_copy(e):
        cols = pl.ds(pl.multiple_of(e * dt2, dt2), dt2)
        return pltpu.make_async_copy(leave(e, 3 * rows, rows), y.at[:, cols], ysem)

    def rounds(xb):
        start(u_copies(0, 0))
        start(u_part(1, 0, 1))
        for i in range(2):
            load_small(xb, i, 0, 0, i)
        barrier = pltpu.get_barrier_semaphore()
        for dev in (fp, fm, sp, sm, sib):
            pl.semaphore_signal(barrier, 1, device_id={"tp": dev})
        pl.semaphore_wait(barrier, 5)

        for hf in range(2):
            hand(0, 0, hf).start()
        for hf in range(2):
            move(source(0, 0, hf), 0, 1, hf, fp).start()
            move(source(0, 0, hf), 0, 2, hf, fm).start()
        inb[...] = jnp.zeros_like(inb)
        for i in range(2, 4):
            load_small(xb, i, 0, 0, i - 2)

        def on(i, v, *calls):
            @when(i == v)
            def _():
                for fn, *a in calls:
                    fn(*a)

        def hook(i):
            on(i, nt - 3, (arrive, 0, 1, 0), (arrive, 0, 2, 0), (load_mid, xb, 0, 0))
            on(i, nt - 1, (load_mid, xb, 1, 0))

        u_small(xb, 0, 0, 0, (0, hr), (row0(0, 0), row0(0, 1)), 0, hook, nt, True, 2)

        def hook(i):
            on(i, 0, (forward, 0, 0))
            on(i, 1, (arrive, 0, 1, 1), (arrive, 0, 2, 1), (forward, 0, 1), (load_mid, xb, 0, 1))

        u_small(xb, 1, 0, 1, (seg, seg + hr), (row0(1, 0), row0(2, 0)), 1, hook, cuts[1], True, 2)
        load_mid(xb, 1, 1)

        def hook(i):
            on(i, 1, (w_pieces, 0, 1))

        u_small(xb, 1, 2 * seg, 2, (half_rows + seg, half_rows + seg + hr), (row0(1, 1), row0(2, 1)), 1, hook, cuts[1], True, 1)

        def hook(i):
            on(i, cuts[1], (w_pieces, 1, 3))
            on(i, nt - 3, (w_pieces, 3, 4))
            on(i, nt - 2, (forward, 0, 2), (push, 1, 0))
            on(i, nt - 1, (push, 1, 1), (load_pair, xb, 0, 0, 0, 1, 0, 0), (load_pair, xb, 0, 1, 0, 1, 0, 1),
               (load_one, xb, 0, 2, 1, 0, 0), (load_one, xb, 0, 3, 1, 0, 1))

        u_big(xb, (seg, half_rows + seg), (row0(1, 0), row0(1, 1)), 1, hook, cuts[1])
        for hf in range(2):
            load_one(xb, 0, 2 + hf, 1, 1, hf)

        def one_round(k, carry):
            fi = 2 // (k + 1)
            first = k == 1

            def up(it, carry):
                b = fi * (it // nt) + (1 - fi) * lax.rem(it, 2)
                i = fi * lax.rem(it, nt) + (1 - fi) * (it // 2)
                ws = lax.rem(i, 2)

                @when(first)
                def _():
                    def keep(c):
                        return (c * seg, half_rows + c * seg)

                    def where(c):
                        return (row0(2 * c, 0), row0(2 * c, 1))

                    def h_parts(c):
                        for part in range(parts - 1):
                            on(it, c * nt + cuts[part + 1], (h_push, hk, 3 + c, part, keep(c), where(c), seg))

                    @when(it < nt)
                    def _():
                        on(it, 0, (h_sent, 0, hr), (far, 1, 0))
                        on(it, 1, (landed, 1, 2), (far, 1, 1))
                        on(it, 2, (give, 1, 2))
                        on(it, 4, (push, 1, 3), (forward, 1, 0), (load_pair, xb, 1, 0, 0, 1, 1, 0), (load_pair, xb, 1, 1, 0, 1, 1, 1),
                           (w_pieces, 4, 6))
                        on(it, 5, (w_pieces, 6, 8), (load_pair, xb, 1, 2, 1, 1, 1, 0), (load_pair, xb, 1, 3, 1, 1, 1, 1))
                        h_parts(0)

                    @when(it >= nt)
                    def _():
                        @when(it < pieces - 2)
                        def _():
                            w_piece(it + 2).start()

                        on(it, nt, (h_push, hk, 3, parts - 1, keep(0), where(0), seg), (h_sent, 1, seg), (forward, 1, 1))
                        on(it, 7, (forward, 1, 2))
                        on(it, 8, (forward, 1, 3))
                        on(it, 9, (push, 2, 0))
                        on(it, 11, (push, 2, 1))
                        h_parts(1)

                @when(k > 1)
                def _():
                    on(it, 2 * nt - 2, (in_start, k - 2, 0))
                    for part in range(1, parts):
                        @when(it == 2 * nt - 3 + part)
                        def _():
                            hy_copy(*cut(part)).start()

                @when(first & (it < 2 * nt - 1))
                def _():
                    start(u_copies(lax.rem(i + 1, nt), 1 - ws))

                @when(it == 2 * nt - 1)
                def _():
                    @when(first)
                    def _():
                        remote(wd, wp, wp_s, wp_r, sib).wait_recv()

                    start(d_copies(0, 0))

                @when(first & (i == 0))
                def _():
                    loaded(xb, b, 0, 4 * seg, b)

                @when(first | (b == 0))
                def _():
                    u_held(0, ws)
                    u_held(1, ws)

                h = hidden(xb.at[b], ws)
                for q in range(4):
                    r = fi * (q * half_rows + b * seg) + (1 - fi) * ((1 - b) * m + q * seg)
                    hk[pl.ds(pl.multiple_of(r, seg), seg), u_cols(i)] = h[q * seg : (q + 1) * seg]
                return carry

            def up_both(i, carry):
                ws = lax.rem(i, 2)
                start(u_copies(i + 1, 1 - ws))

                @when(k == 2)
                def _():
                    on(i, 0, (h_sent, 3, seg), (h_sent, 4, seg))
                    on(i, 2, (push, 3, 0))
                    on(i, 4, (push, 3, 1))

                @when(k == 3)
                def _():
                    on(i, 4, (push, 0, 3))

                    @when(i == 0)
                    def _():
                        hy_all().wait_send()

                @when(i == cuts[1])
                def _():
                    pl.semaphore_wait(hfree, 1)
                    hy_copy(*cut(0)).start()

                @when(i == 0)
                def _():
                    for slot in range(2):
                        loaded(xb, slot, 0, 4 * seg, slot)

                u_held(0, ws)
                u_held(1, ws)
                hk[pl.ds(m, m), u_cols(i)] = hidden(xb.at[0], ws)
                hk[pl.ds(0, m), u_cols(i)] = hidden(xb.at[1], ws)
                return carry

            lax.fori_loop(0, (1 - fi) * (nt - 1), up_both, 0)
            lax.fori_loop((1 - fi) * 2 * (nt - 1), 2 * nt, up, 0)

            @when(first)
            def _():
                h_push(hk, 4, parts - 1, (seg, half_rows + seg), (row0(2, 0), row0(2, 1)), seg)
                h_here(3, seg)
                h_here(4, seg)

            @when(k > 1)
            def _():
                hy_all().wait_recv()

            def down(n, carry):
                ws = lax.rem(n, 2)

                @when(n < nd - 1)
                def _():
                    start(d_copies(n + 1, 1 - ws))

                @when(n == nd - 1)
                def _():
                    start(u_copies(0, 0))

                @when(k > 1)
                def _():
                    in_copy(k - 2, n).wait()

                    @when(n < nd - 1)
                    def _():
                        in_start(k - 2, n + 1)

                    sum_all(0, n).wait_send()

                @when(first)
                def _():
                    on(n, 1, (push, 2, 2))
                    on(n, 4, (push, 2, 3))

                    @when(lax.rem(n, 2) == 0)
                    def _():
                        forward(2, n // 2)

                @when(k == 2)
                def _():
                    on(n, 2, (push, 3, 2))
                    on(n, 4, (push, 3, 3))
                    on(n, 7, (far, 0, 0), (far, 0, 1))

                @when((k < 3) & ((n == 1) | (n == 3) | (n == 5) | (n == 6)))
                def _():
                    other, pair = lax.rem(n // 2, 2), n // (nd // 2)
                    for hf in range(2):
                        load_pair(xb, 1 - other, 2 * hf + pair, other, k + 1, pair, hf)

                @when(k == 3)
                def _():
                    for q in range(4):
                        on(n, 2 + q, (load_small, xb, q, 0, 3, q % 2))

                d_held(ws)
                for q in range(sub):
                    total, cols = products(hk.at[pl.ds(0, m)], n, q)
                    out[n, :, cols] = total.astype(BF16)
                for hf in range(2):
                    sum_copy(k - 1, n, hf).start()
                return carry

            lax.fori_loop(0, nd, down, 0)

            @when(k < 3)
            def _():
                pl.semaphore_signal(hfree, 1, device_id={"tp": sib})

            return carry

        lax.fori_loop(1, side, one_round, 0)

        def hook(i):
            on(i, nt - 2, (in_start, 2, 0))

        hy_all().wait_send()
        u_small(xb, 0, 0, 0, (0, hr), (row0(3, 0), row0(3, 1)), 5, hook, nt, False, 0)

    pl.run_scoped(rounds, pltpu.VMEM((2, 8 * hr, d), BF16))

    def last(t0, t1, t2):
        h_sent(5, hr)
        for dev in (fp, fm):
            pl.semaphore_signal(nfree, 1, device_id={"tp": dev})
        for idx, size in ((0, hr), (1, seg), (5, hr)):
            h_here(idx, size)

        def add_far(e):
            both = pl.ds(0, rows)
            remote(out.at[0, both, pl.ds(0, dt2)], land(e, 2), a_s, a_r.at[e], fp).wait_recv()
            far_in = land(e, 2)[...].astype(F32)
            leave(e, rows, hr)[...] = (t2[e, :hr] + far_in[:hr]).astype(BF16)
            leave(e, rows + hr, hr)[...] = t2[e, hr:].astype(BF16)
            leave(e, 2 * rows, hr)[...] = t1[e, :hr].astype(BF16)
            leave(e, 2 * rows + hr, hr)[...] = (t1[e, hr:] + far_in[hr:]).astype(BF16)
            for i in range(2):
                b_copy(e, i).start()

        def add_near(e):
            both = pl.ds(0, 2 * rows)
            remote(out.at[0, both, pl.ds(0, dt2)], out.at[0, both, pl.ds(0, dt2)], b_s, b_r.at[e], fp).wait_recv()
            leave(e, 3 * rows, rows)[...] = (t0[e] + land(e, 0)[...].astype(F32) + land(e, 1)[...].astype(F32)).astype(BF16)
            y_copy(e).start()

        def down(e, carry):
            n, c2 = e // 2, lax.rem(e, 2)
            ws = lax.rem(n, 2)

            @when(c2 == 0)
            def _():
                @when(n < nd - 1)
                def _():
                    start(d_copies(n + 1, 1 - ws))

                in_copy(2, n).wait()

                @when(n < nd - 1)
                def _():
                    in_start(2, n + 1)

                sum_all(0, n).wait_send()
                d_held(ws)

            @when(e >= 3)
            def _():
                add_far(e - 3)

            @when(e >= 6)
            def _():
                add_near(e - 6)

            for q in range(2):
                term = jnp.dot(h0[...], wbuf[ws, pl.ds(pl.multiple_of(c2 * 2 * hid, 2 * hid), 2 * hid), q * tn : (q + 1) * tn], preferred_element_type=F32)
                cols = slice(q * tn, (q + 1) * tn)
                total = term + inb[lax.rem(n, 2), :, pl.ds(pl.multiple_of(c2 * dt2 + q * tn, tn), tn)].astype(F32)
                for hf in range(2):
                    o = hf * half_rows
                    dst = pl.ds(hf * hr, hr)
                    t0[e, dst, cols] = total[o : o + hr]
                    t1[e, dst, cols] = total[o + hr : o + 2 * hr]
                    t2[e, dst, cols] = total[o + 2 * hr : o + 3 * hr]
                    out[n, dst, pl.ds(pl.multiple_of(c2 * dt2 + q * tn, tn), tn)] = total[o + 3 * hr : o + 4 * hr].astype(BF16)

            @when(e == 0)
            def _():
                pl.semaphore_wait(nfree, 2)

            for hf in range(2):
                a_copy(e, hf).start()
            return carry

        lax.fori_loop(0, ne, down, 0)
        for i in range(3):
            add_near(ne - 6 + i)
            add_far(ne - 3 + i)
        for i in range(3):
            add_near(ne - 3 + i)

    shape = pltpu.VMEM((ne, rows, dt2), F32)
    pl.run_scoped(last, shape, shape, shape)

    pltpu.make_async_copy(y, y, ysem).wait()
    for sem, r in ((a_s, pl.ds(0, rows)), (b_s, pl.ds(rows, 2 * rows))):
        remote(out.at[:, r], out.at[:, r], sem, a_r.at[0], fp).wait_send()
    remote(wd, wp, wp_s, wp_r, sib).wait_send()
    remote(xs.at[1], xs.at[1], pu_s, pu_r.at[0, 0], sib).wait_send()
    sent = xs.at[0, :, pl.ds(0, 2 * (side * side - 1) * hr // side)]
    remote(sent, sent, ag_s, ag_r.at[0, 2], fp).wait_send()


def build(mesh, tn, dt):
    side = math.isqrt(mesh.shape["tp"] // 2)

    def step(x, w_gate, w_up, w_down):
        rows, d = x.shape
        hid = w_gate.shape[1]
        hr = rows // 2
        nt, nd = hid // tn, d // dt
        dma = pltpu.SemaphoreType.DMA
        hbm = pl.BlockSpec(memory_space=pltpu.HBM)
        m = side * rows
        result = pl.pallas_call(
            functools.partial(kernel, side, tn, dt),
            out_shape=(
                jax.ShapeDtypeStruct((rows, d), BF16),
                jax.ShapeDtypeStruct((2, side, m, d), BF16),
                jax.ShapeDtypeStruct((hid, d), BF16),
                jax.ShapeDtypeStruct((side - 1, nd, m, dt), BF16),
            ),
            in_specs=[hbm] * 4,
            out_specs=[hbm] * 4,
            scratch_shapes=[
                pltpu.VMEM((2, d, 2 * tn), BF16),
                pltpu.VMEM((m, 2 * hid), BF16),
                pltpu.VMEM((2 * m, 2 * hid), BF16),
                pltpu.VMEM((nd, m, dt), BF16),
                pltpu.VMEM((2, m, dt), BF16),
                dma((2, 2)),
                dma((3,)),
                dma((2,)),
                dma,
                dma,
                dma((side, 2 * side)),
                dma,
                dma((side, 2 * side)),
                dma,
                dma,
                dma((6,)),
                dma((6,)),
                dma,
                dma,
                dma((nd,)),
                dma((side - 1, nd)),
                dma,
                dma((2 * nd,)),
                dma,
                dma((2 * nd,)),
                pltpu.SemaphoreType.REGULAR,
                pltpu.SemaphoreType.REGULAR,
            ],
            compiler_params=pltpu.CompilerParams(collective_id=0, has_side_effects=True, vmem_limit_bytes=67043328),
            cost_estimate=pl.CostEstimate(flops=6 * side * side * 2 * rows * d * hid, bytes_accessed=9 * d * hid * 4, transcendentals=0),
            name="mlp",
        )(x, w_gate, w_up, w_down)
        return result[0]

    return jax.shard_map(
        step,
        mesh=mesh,
        in_specs=(P(("dp", "tp"), None), P(None, "tp"), P(None, "tp"), P("tp", None)),
        out_specs=P(("dp", "tp"), None),
        check_vma=False,
    )


def solution(mesh):
    return build(mesh, 256, 1024)
```
